32 devices in a mesh: tm: 8 (over z, x), env: 4 (over y, core).
Axes of the slice: x: 2, y: 2, z: 4, core: 2. Of those that a mesh axis runs over, the one named last changes fastest.
Arguments:
- init_state: float32 [70, 1024], P(None, 'env'), may hold values from -6 to 6
- torque: float32 [32, 35, 1024], P('tm', None, 'env'), may hold values from -192 to 192
- contact: int32 [32, 1024], P('tm', 'env'), may hold values 0 or 1
- mass_inverse: float32 [16, 35, 35], P('tm'), may hold values from -0.014 to 1.5, as said below
- stiffness: float32 [35], replicated, may hold values from 10 to 100
- damping: float32 [35], replicated, may hold values from 0.5 to 5
- gravity: float32 [35], replicated, may hold values from 1 to 10
- contact_stiffness: float32 [35], replicated, may hold values from 20 to 100
- contact_damping: float32 [35], replicated, may hold values from 0.5 to 3
Outputs:
- final_states: float32 [16, 70, 1024], P('tm', None, 'env')
- corrections: float32 [3, 1024], P(None, 'env')
The draws below stay inside these ranges and needn't reach their ends.
Inputs may be any that keep to these rules, and one draw needn't show every extreme that they name: `mass_inverse`: each matrix is symmetric, and each diagonal entry exceeds the sum of the magnitudes of the other entries of its row.
All inputs are finite; a program needn't handle non-finite values. No bound on the sum of `contact` on one device may be relied on, other than what follows from the above.
Results may differ from the reference program's by a relative error of at most 0.00025.
Values sent between devices are 32-bit elements; how exact they have to be, the bound alone decides.
A program may use at most 64 MiB of HBM per device.

```python
import math
import jax
import jax.numpy as jnp
from jax import lax

DOF = 35
STATE = 70
HS = 2
SUB = 32
ITERS = 3
SLICES = 16
STEPS = 32
ENV = 1024


def draw_mass_inverse(key, part):
    key_diag = jax.random.fold_in(key, 11)
    key_off = jax.random.fold_in(key, 12)
    diagonal = jax.random.uniform(key_diag, (SLICES, DOF), jnp.float32, 0.5, 1.5)
    raw = jnp.clip(0.008 * jax.random.normal(key_off, (SLICES, DOF, DOF), jnp.float32), -0.014, 0.014)
    upper = jnp.triu(raw, 1)
    return upper + jnp.swapaxes(upper, 1, 2) + diagonal[:, :, None] * jnp.eye(DOF, dtype=jnp.float32)


def touch_ends(values, own_key, low, largest):
    spot = [jax.random.randint(jax.random.fold_in(own_key, axis), (), 0, length) for axis, length in enumerate(values.shape)]
    widest = values.shape.index(max(values.shape))
    neighbour = spot[:widest] + [(spot[widest] + 1) % values.shape[widest]] + spot[widest + 1:]
    return values.at[tuple(spot)].set(low).at[tuple(neighbour)].set(largest)


def shard_levels(key, extent, cuts, low, largest):
    factor_of, own = 1.0, jax.random.fold_in(key, 6)
    for position, shards_of in cuts:
        draws = jnp.exp(jax.random.uniform(jax.random.fold_in(own, position), (shards_of,), jnp.float32, low / len(cuts), largest / len(cuts)))
        factor_of = factor_of * jnp.repeat(draws, extent[position] // shards_of).reshape([-1 if axis == position else 1 for axis in range(len(extent))])
    return factor_of


def gaussian(own_key, dims, deviation, most, shards=(), kind=jnp.bfloat16):
    array = jax.random.normal(own_key, dims, jnp.float32) * deviation
    if len(shards) > 0:
        array = shard_levels(own_key, dims, shards, -0.22, 0.18) * array
    return jnp.clip(array, min=-most, max=most).astype(kind)


def setup_inputs(seed: int = 0) -> dict:
    arg_keys = jax.random.split(jax.random.key(seed), 10)
    return {
        "init_state": gaussian(arg_keys[0], (STATE, ENV), 0.5, 6.0, ((1, 4),), jnp.float32),
        "torque": gaussian(arg_keys[1], (STEPS, DOF, ENV), 30.0, 192.0, ((0, 8), (2, 4)), jnp.float32),
        "contact": touch_ends((jax.random.randint(arg_keys[2], (STEPS, ENV), 0, 3) < 1).astype(jnp.int32), jax.random.fold_in(arg_keys[2], 1), 0, 1),
        "mass_inverse": draw_mass_inverse(jax.random.fold_in(arg_keys[9], 71), 0),
        "stiffness": jnp.clip(jnp.exp(jax.random.uniform(arg_keys[4], (DOF,), jnp.float32, math.log(10.0), math.log(100.0))), 10.0, 100.0),
        "damping": jnp.clip(jnp.exp(jax.random.uniform(arg_keys[5], (DOF,), jnp.float32, math.log(0.5), math.log(5.0))), 0.5, 5.0),
        "gravity": jnp.clip(jnp.exp(jax.random.uniform(arg_keys[6], (DOF,), jnp.float32, math.log(1.0), math.log(10.0))), 1.0, 10.0),
        "contact_stiffness": jnp.clip(jnp.exp(jax.random.uniform(arg_keys[7], (DOF,), jnp.float32, math.log(20.0), math.log(100.0))), 20.0, 100.0),
        "contact_damping": jnp.clip(jnp.exp(jax.random.uniform(arg_keys[8], (DOF,), jnp.float32, math.log(0.5), math.log(3.0))), 0.5, 3.0),
    }


step_length = 0.05

def exact_dot(left, right):
    return jnp.dot(left, right, precision=lax.Precision.HIGHEST, preferred_element_type=jnp.float32)

def coarse_one(state_now, torque_steps, mean_steps, inverse, params):
    stiffness, damping, gravity, contact_stiffness, contact_damping = params
    joint_pos = state_now[:DOF]
    joint_vel = state_now[DOF:]
    for step_pos in range(HS):
        spring = (stiffness + gravity + mean_steps[step_pos] * contact_stiffness)[:, None]
        friction = (damping + mean_steps[step_pos] * contact_damping)[:, None]
        force = torque_steps[step_pos] - spring * joint_pos - friction * joint_vel
        joint_vel = joint_vel + step_length * exact_dot(inverse, force)
        joint_pos = joint_pos + step_length * joint_vel
    return jnp.concatenate([joint_pos, joint_vel], axis=0)

def fine_one(state_now, torque_steps, contact_steps, inverse, params):
    stiffness, damping, gravity, contact_stiffness, contact_damping = params
    fine_dt = step_length / SUB
    joint_pair = (state_now[:DOF], state_now[DOF:])
    for step_pos in range(HS):
        torque_here = torque_steps[step_pos]
        contact_here = contact_steps[step_pos][None, :]

        def substep(counter, pair_now):
            joint_pos, joint_vel = pair_now
            force = torque_here - stiffness[:, None] * joint_pos - damping[:, None] * joint_vel - gravity[:, None] * jnp.sin(joint_pos) - contact_here * (contact_stiffness[:, None] * joint_pos + contact_damping[:, None] * joint_vel)
            joint_vel = joint_vel + fine_dt * exact_dot(inverse, force)
            joint_pos = joint_pos + fine_dt * joint_vel
            return (joint_pos, joint_vel)
        joint_pair = lax.fori_loop(0, SUB, substep, joint_pair)
    return jnp.concatenate([joint_pair[0], joint_pair[1]], axis=0)

def reference(init_state, torque, contact, mass_inverse, stiffness, damping, gravity, contact_stiffness, contact_damping):
    params = (stiffness, damping, gravity, contact_stiffness, contact_damping)
    torque_steps = torque.reshape(SLICES, HS, DOF, ENV)
    contact_steps = contact.astype(jnp.float32).reshape(SLICES, HS, ENV)
    mean_steps = lax.optimization_barrier(jnp.mean(contact_steps, axis=2))
    coarse_all = jax.vmap(coarse_one, in_axes=(0, 0, 0, 0, None))
    fine_all = jax.vmap(fine_one, in_axes=(0, 0, 0, 0, None))

    def chain(jumps):

        def advance(state_now, inputs):
            torque_here, mean_here, inverse, jump = inputs
            following = coarse_one(state_now, torque_here, mean_here, inverse, params) + jump
            return (following, following)
        unused, ends = lax.scan(advance, init_state, (torque_steps, mean_steps, mass_inverse, jumps))
        return ends
    ends = chain(jnp.zeros((SLICES, STATE, ENV), jnp.float32))
    records = []
    for iteration in range(ITERS):
        starts = jnp.concatenate([init_state[None], ends[:-1]], axis=0)
        jumps = fine_all(starts, torque_steps, contact_steps, mass_inverse, params) - coarse_all(starts, torque_steps, mean_steps, mass_inverse, params)
        new_ends = chain(jumps)
        records.append(lax.optimization_barrier(jnp.max(jnp.sqrt(lax.optimization_barrier(jnp.sum((new_ends - ends) ** 2, axis=1))), axis=0)))
        ends = new_ends
    return (ends, jnp.stack(records))
```

```python
import functools
import math

import jax
import jax.numpy as jnp
from jax import lax
from jax.experimental import pallas as pl
from jax.experimental.pallas import tpu as pltpu
from jax.sharding import PartitionSpec as P

DOF = 35
HS = 2
SUB = 32
ITERS = 3
LANES = 128
WIDE = 256
VOFF = -(-DOF // 8) * 8
DEPTH = 2 * VOFF
PER = LANES // DOF
SPARE = PER * DOF

step_length = 0.05
fine_dt = step_length / SUB
TWO_PI = 2.0 * math.pi
MESH = pl.DeviceIdType.MESH
F32 = jnp.float32
BF16 = jnp.bfloat16

SIN = (
    6.283182818551188, -41.341421398631915, 81.59618387021051,
    -76.58010048603072, 41.205394649903326, -12.271261959178284,
)


def up8(n):
    return -(-n // 8) * 8


def split(value):
    high = value.astype(BF16)
    return high, (value - high.astype(F32)).astype(BF16)


def dot(left, right):
    return jnp.dot(left, right, preferred_element_type=F32)


class Plan:
    def __init__(self, slices):
        per = PER
        self.groups = []
        self.where = []
        base = 0
        for first in range(0, slices, per):
            count = min(per, slices - first)
            width = -(-count * DOF // LANES) * LANES
            self.groups.append((base, width, first, count))
            for pos in range(count):
                self.where.append(base + pos * DOF)
            base += width
        self.lanes = base


class Message:
    def __init__(self, steps, local, epd):
        self.steps, self.local, self.epd = steps, local, epd
        count = steps + local
        self.tiles = -(-count // PER)
        self.rows = []
        self.start = []
        base = 0
        for tile in range(self.tiles):
            pieces = range(tile * PER, min(count, (tile + 1) * PER))
            tall = any(i >= steps for i in pieces)
            rows = max(up8(epd), up8(DOF)) if tall else up8(epd)
            self.start.append(base)
            self.rows.append(rows)
            base += rows
        self.total = base

    def place(self, piece):
        tile, pos = divmod(piece, PER)
        return self.start[tile], pos * DOF


def kernel(
    tm, env, local, total_env,
    init, torque, contact, minv, stiff_r, damp_r, gravity_r, cstiff_r, cdamp_r,
    states_out, corr_out,
    tx, rx, row, rows, srow, sums, otx, orx, turn, mtile, own,
    tq, spring, fric, grav, cspring, cfric, wgt, wtmp, ybuf, ubuf, by, bu, ly, lu, cmap, pmap, ctmp, xs,
    tsend, trecv, esend, erecv, ssend, srecv, osend, orecv,
):
    slices = local * tm
    steps = local * HS
    env_local = contact.shape[1]
    epd = env_local // tm
    plan = Plan(slices)
    msg = Message(steps, local, epd)
    me_t = lax.axis_index("tm")
    me_e = lax.axis_index("env")
    barrier = pltpu.get_barrier_semaphore()

    def tm_peer(k):
        return {"tm": lax.rem(me_t + k, tm), "env": me_e}

    def env_peer(k):
        return {"tm": me_t, "env": lax.rem(me_e + k, env)}

    for k in range(1, env):
        pl.semaphore_signal(barrier, inc=1, device_id=env_peer(k), device_id_type=MESH)
    for k in range(1, tm):
        pl.semaphore_signal(barrier, inc=1, device_id=tm_peer(k), device_id_type=MESH)

    hits = contact[...].astype(F32)
    row[...] = jnp.zeros(row.shape, F32)
    row[0:steps, :] = jnp.broadcast_to(jnp.sum(hits, axis=1, keepdims=True), (steps, LANES))
    for tile in range(msg.tiles):
        turn[...] = jnp.zeros(turn.shape, F32)
        mtile[...] = jnp.zeros(mtile.shape, F32)
        for pos in range(PER):
            piece = tile * PER + pos
            if piece < steps:
                turn[pos * DOF : (pos + 1) * DOF, :] = torque[:, piece, :]
            elif piece < steps + local:
                mtile[0:DOF, pos * DOF : (pos + 1) * DOF] = minv[:, piece - steps, :]
        if tile == 0:
            turn[SPARE : SPARE + steps, :] = hits
        turned = turn[...].T
        first, count = msg.start[tile], msg.rows[tile]
        tall = count > up8(epd) or any(
            steps <= i < steps + local for i in range(tile * PER, (tile + 1) * PER))
        for p in range(tm):
            chunk = turned[p * epd : (p + 1) * epd]
            if tall:
                tx[p, first : first + count, :] = mtile[0:count, :]
                tx[p, first : first + epd, :] = tx[p, first : first + epd, :] + chunk
            else:
                tx[p, first : first + epd, :] = chunk
    turn[...] = jnp.zeros(turn.shape, F32)
    turn[0:DOF, :] = init[0:DOF, :]
    turn[VOFF : VOFF + DOF, :] = init[DOF : 2 * DOF, :]
    turned = turn[...].T
    for p in range(tm):
        own[p] = turned[p * epd : (p + 1) * epd]

    pl.semaphore_wait(barrier, tm + env - 2)

    def row_copy(k):
        return pltpu.make_async_remote_copy(
            src_ref=row, dst_ref=rows.at[me_e], send_sem=esend.at[k], recv_sem=erecv.at[k],
            device_id=env_peer(k), device_id_type=MESH)

    def block_copy(k):
        return pltpu.make_async_remote_copy(
            src_ref=tx.at[lax.rem(me_t + k, tm)], dst_ref=rx.at[me_t],
            send_sem=tsend.at[k], recv_sem=trecv.at[k],
            device_id=tm_peer(k), device_id_type=MESH)

    def sum_copy(k):
        return pltpu.make_async_remote_copy(
            src_ref=srow, dst_ref=sums.at[me_t], send_sem=ssend.at[k], recv_sem=srecv.at[k],
            device_id=tm_peer(k), device_id_type=MESH)

    def out_copy(k):
        return pltpu.make_async_remote_copy(
            src_ref=otx.at[lax.rem(me_t + k, tm)], dst_ref=orx.at[me_t],
            send_sem=osend.at[k], recv_sem=orecv.at[k],
            device_id=tm_peer(k), device_id_type=MESH)

    row_copies = [row_copy(k) for k in range(1, env)]
    block_copies = [block_copy(k) for k in range(1, tm)]
    sum_copies = [sum_copy(k) for k in range(1, tm)]
    for c in row_copies + block_copies:
        c.start()
    rows[me_e] = row[...]
    rx[me_t] = tx[me_t]

    stiff, damp, gravity, cstiff, cdamp = (
        r[...] for r in (stiff_r, damp_r, gravity_r, cstiff_r, cdamp_r))
    ratio = float(SUB)
    block = 4 if slices % 4 == 0 else 1
    unroll = max(1, min(SUB, 96 // len(plan.groups)))
    to_u = TWO_PI / fine_dt
    for ref in (tq, spring, fric, grav, cspring, cfric, ybuf, ubuf, ly, lu):
        ref[...] = jnp.zeros(ref.shape, ref.dtype)
    ctmp[...] = jnp.zeros(ctmp.shape, F32)
    xs[...] = jnp.zeros(xs.shape, F32)
    cmap[...] = jnp.zeros(cmap.shape, BF16)
    rank = lax.broadcasted_iota(jnp.int32, (DEPTH, DOF), 0)
    col = lax.broadcasted_iota(jnp.int32, (DEPTH, DOF), 1)
    for n in range(slices):
        cut = pl.ds(plan.where[n], DOF)
        grav[:, cut] = gravity
        ly[:, cut] = jnp.where(rank == col, 1.0, 0.0)
        lu[:, cut] = jnp.where(rank == col + VOFF, 1.0, 0.0)

    for c in row_copies:
        c.wait()
    srow[...] = jnp.sum(rows[...], axis=0) * (1.0 / total_env)
    for c in sum_copies:
        c.start()
    sums[me_t] = srow[...]
    for c in block_copies:
        c.wait()

    for n in range(slices):
        src, pos = divmod(n, local)
        cut = pl.ds(plan.where[n], DOF)
        for j in range(HS):
            step = pos * HS + j
            first, lane = msg.place(step)
            hit = rx[src, 0:epd, SPARE + step : SPARE + step + 1]
            tq[j, :, cut] = rx[src, first : first + epd, lane : lane + DOF]
            spring[j, :, cut] = TWO_PI * (stiff + hit * cstiff)
            fric[j, :, cut] = to_u * (damp + hit * cdamp)

    for g, (base, width, first, count) in enumerate(plan.groups):
        wtmp[...] = jnp.zeros(wtmp.shape, F32)
        for pos in range(count):
            src, here = divmod(first + pos, local)
            start, lane = msg.place(steps + here)
            wtmp[pl.ds(pos * DOF, DOF), pl.ds(pos * DOF, DOF)] = (
                fine_dt * fine_dt / TWO_PI
            ) * rx[src, start : start + DOF, lane : lane + DOF]
        high, low = split(wtmp[...])
        wgt[g, 0:LANES, 0:LANES] = high
        wgt[g, LANES:, 0:LANES] = high
        wgt[g, 0:LANES, LANES:] = low
        wgt[g, LANES:, LANES:] = jnp.zeros_like(low)

    for c in sum_copies:
        c.wait()
    for n in range(slices):
        src, pos = divmod(n, local)
        cut = pl.ds(plan.where[n], DOF)
        for j in range(HS):
            step = pos * HS + j
            mean = sums[src, step : step + 1, 0:DOF]
            cspring[j, :, cut] = TWO_PI * (stiff + gravity + mean * cstiff)
            cfric[j, :, cut] = to_u * (damp + mean * cdamp)

    def product(force, g):
        high, low = split(force)
        both = dot(jnp.concatenate([high, low], axis=1), wgt[g])
        return both[:, :LANES] + both[:, LANES:]

    for g, (base, width, first, count) in enumerate(plan.groups):
        cut = pl.ds(base, width)
        y, u = ly[:, cut], lu[:, cut]
        for j in range(HS):
            force = -cspring[j, :, cut] * y - cfric[j, :, cut] * u
            u = u + ratio * product(force, g)
            y = y + ratio * u
        ly[:, cut] = y
        lu[:, cut] = u
        u = ratio * product(tq[0, :, cut], g)
        y = ratio * u
        for j in range(1, HS):
            force = tq[j, :, cut] - cspring[j, :, cut] * y - cfric[j, :, cut] * u
            u = u + ratio * product(force, g)
            y = y + ratio * u
        by[:, cut] = y
        bu[:, cut] = u
    for n in range(slices):
        cut = pl.ds(plan.where[n], DOF)
        ctmp[0:DEPTH, 0:DOF] = ly[:, cut]
        ctmp[0:DEPTH, VOFF : VOFF + DOF] = lu[:, cut]
        high, low = split(ctmp[...])
        cmap[n, 0:LANES, 0:LANES] = high
        cmap[n, LANES:, 0:LANES] = high
        cmap[n, 0:LANES, LANES:] = low

    def through(state, weight):
        high, low = split(state)
        both = dot(jnp.concatenate([high, low], axis=1), weight)
        return both[:, :LANES] + both[:, LANES:]

    def joined(y, u, depth):
        gap = jnp.zeros((depth, VOFF - DOF), F32)
        return jnp.concatenate(
            [y, gap, u, jnp.zeros((depth, LANES - VOFF - DOF), F32)], axis=1)

    firsts = range(0, slices, block)
    running = {m: joined(ly[:, pl.ds(plan.where[m], DOF)], lu[:, pl.ds(plan.where[m], DOF)], DEPTH)
               for m in firsts}
    for i in range(1, block):
        for m in firsts:
            running[m] = through(running[m], cmap[m + i])
            ctmp[0:DEPTH, :] = running[m]
            high, low = split(ctmp[...])
            pmap[m + i, 0:LANES, 0:LANES] = high
            pmap[m + i, LANES:, 0:LANES] = high
            pmap[m + i, 0:LANES, LANES:] = low
            pmap[m + i, LANES:, LANES:] = jnp.zeros_like(low)

    def sweep(offsets, entry):
        ends = list(offsets)
        for i in range(1, block):
            for m in firsts:
                ends[m + i] = through(ends[m + i - 1], cmap[m + i]) + ends[m + i]
        enter = {}
        for m in firsts:
            enter[m] = entry
            last = m + block - 1
            whole = pmap if block > 1 else cmap
            if entry is not None:
                ends[last] = ends[last] + through(entry, whole[last])
            entry = ends[last]
        for i in range(block - 1):
            for m in firsts:
                if enter[m] is not None:
                    part = cmap if i == 0 else pmap
                    ends[m + i] = ends[m + i] + through(enter[m], part[m + i])
        return ends

    def packed(yref, uref, n):
        cut = pl.ds(plan.where[n], DOF)
        return joined(yref[:, cut], uref[:, cut], epd)

    lane_of = lax.broadcasted_iota(jnp.int32, (1, LANES), 1)
    scale = jnp.where(lane_of < VOFF, TWO_PI, to_u)
    shrink = jnp.where(lane_of < VOFF, 1.0 / TWO_PI, 1.0 / to_u)
    state = own[me_t] * shrink
    xs[0] = state
    ends = sweep([packed(by, bu, n) for n in range(slices)], state)
    for n in range(slices):
        xs[n + 1] = ends[n]

    def iteration(k, corrections):
        for n in range(slices):
            cut = pl.ds(plan.where[n], DOF)
            ybuf[:, cut] = xs[n, :, 0:DOF]
            ubuf[:, cut] = xs[n, :, VOFF : VOFF + DOF]
        for j in range(HS):

            def substep(counter, carry):
                result = []
                for g, (base, width, first, count) in enumerate(plan.groups):
                    y, u = carry[g]
                    cut = pl.ds(base, width)
                    t = y - jnp.round(y)
                    s = t * t
                    poly = jnp.full_like(s, SIN[-1])
                    for c in SIN[-2::-1]:
                        poly = poly * s + c
                    force = (
                        tq[j, :, cut]
                        - spring[j, :, cut] * y
                        - fric[j, :, cut] * u
                        - (grav[:, cut] * t) * poly
                    )
                    u = u + product(force, g)
                    y = y + u
                    result.append((y, u))
                return tuple(result)

            first_state = tuple(
                (ybuf[:, pl.ds(base, width)], ubuf[:, pl.ds(base, width)])
                for base, width, first, count in plan.groups
            )
            last = lax.fori_loop(0, SUB, substep, first_state, unroll=unroll)
            for g, (base, width, first, count) in enumerate(plan.groups):
                ybuf[:, pl.ds(base, width)] = last[g][0]
                ubuf[:, pl.ds(base, width)] = last[g][1]
        worst = jnp.zeros((epd, 1), F32)
        changes = sweep([packed(ybuf, ubuf, n) - xs[n + 1] for n in range(slices)], None)
        for n in range(slices):
            real = changes[n] * scale
            worst = jnp.maximum(worst, jnp.sum(real * real, axis=1, keepdims=True))
            xs[n + 1] = xs[n + 1] + changes[n]
        return jnp.where(lane_of == DOF + k, jnp.sqrt(worst), corrections)

    corrections = lax.fori_loop(0, ITERS, iteration, jnp.zeros((epd, LANES), F32))

    span = local * epd
    for t in range(tm):
        parts = [xs[t * local + pos + 1] * scale for pos in range(local)]
        parts[0] = parts[0] + corrections
        turned = jnp.concatenate(parts, axis=0).T
        otx[t, :, 0:span] = turned[0:VOFF]
        otx[t, :, span : 2 * span] = turned[VOFF:DEPTH]
    out_copies = [out_copy(k) for k in range(1, tm)]
    for c in out_copies:
        c.start()
    orx[me_t] = otx[me_t]
    for c in out_copies:
        c.wait()

    across = LANES // epd
    lanes = lax.broadcasted_iota(jnp.int32, (VOFF, LANES), 1)
    for part in range(2):
        for pos in range(local):
            off = part * span + pos * epd
            for tile in range(env_local // LANES):
                acc = None
                for q in range(across):
                    block_in = orx[tile * across + q]
                    shift = (q * epd - off) % LANES
                    moved = pltpu.roll(block_in, shift, 1) if shift else block_in
                    acc = moved if acc is None else jnp.where(lanes >= q * epd, moved, acc)
                cut = pl.ds(tile * LANES, LANES)
                states_out[part * DOF : (part + 1) * DOF, pos, cut] = acc[0:DOF]
                if part == 0 and pos == 0:
                    corr_out[:, cut] = acc[DOF : DOF + ITERS]


def body(tm, env, init_state, torque, contact, mass_inverse, stiffness, damping, gravity,
         contact_stiffness, contact_damping):
    local = mass_inverse.shape[0]
    env_local = init_state.shape[1]
    epd = env_local // tm
    steps = local * HS
    slices = local * tm
    plan = Plan(slices)
    msg = Message(steps, local, epd)
    vmem = pl.BlockSpec(memory_space=pltpu.VMEM)
    dma = pltpu.SemaphoreType.DMA
    prm = [p.reshape(1, DOF) for p in (stiffness, damping, gravity, contact_stiffness, contact_damping)]
    lanes = plan.lanes
    groups = len(plan.groups)
    big = pltpu.VMEM((epd, lanes), F32)
    both = pltpu.VMEM((HS, epd, lanes), F32)
    thin = pltpu.VMEM((HS, 1, lanes), F32)
    row = (up8(steps), LANES)
    states, corrections = pl.pallas_call(
        functools.partial(kernel, tm, env, local, env_local * env),
        out_shape=(
            jax.ShapeDtypeStruct((2 * DOF, local, env_local), F32),
            jax.ShapeDtypeStruct((ITERS, env_local), F32),
        ),
        in_specs=[vmem] * 9,
        out_specs=(vmem, vmem),
        scratch_shapes=[
            pltpu.VMEM((tm, msg.total, LANES), F32), pltpu.VMEM((tm, msg.total, LANES), F32),
            pltpu.VMEM(row, F32), pltpu.VMEM((env,) + row, F32),
            pltpu.VMEM(row, F32), pltpu.VMEM((tm,) + row, F32),
            pltpu.VMEM((tm, VOFF, LANES), F32), pltpu.VMEM((tm, VOFF, LANES), F32),
            pltpu.VMEM((LANES, env_local), F32),
            pltpu.VMEM((max(msg.rows), LANES), F32),
            pltpu.VMEM((tm, epd, LANES), F32),
            both, both, both, pltpu.VMEM((1, lanes), F32), thin, thin,
            pltpu.VMEM((groups, WIDE, WIDE), BF16),
            pltpu.VMEM((LANES, LANES), F32),
            big, big, big, big,
            pltpu.VMEM((DEPTH, lanes), F32), pltpu.VMEM((DEPTH, lanes), F32),
            pltpu.VMEM((slices, 2 * LANES, 2 * LANES), BF16),
            pltpu.VMEM((slices, 2 * LANES, 2 * LANES), BF16),
            pltpu.VMEM((LANES, LANES), F32),
            pltpu.VMEM((slices + 1, epd, LANES), F32),
            dma((tm,)), dma((tm,)), dma((env,)), dma((env,)),
            dma((tm,)), dma((tm,)), dma((tm,)), dma((tm,)),
        ],
        compiler_params=pltpu.CompilerParams(collective_id=0, has_side_effects=True),
        name="parareal",
    )(init_state, jnp.transpose(torque, (1, 0, 2)), contact,
      jnp.transpose(mass_inverse, (1, 0, 2)), *prm)
    return jnp.transpose(states, (1, 0, 2)), corrections


def solution(mesh):
    placed = (
        P(None, "env"),
        P("tm", None, "env"),
        P("tm", "env"),
        P("tm", None, None),
        P(),
        P(),
        P(),
        P(),
        P(),
    )
    return jax.shard_map(
        functools.partial(body, mesh.shape["tm"], mesh.shape["env"]),
        mesh=mesh,
        in_specs=placed,
        out_specs=(P("tm", None, "env"), P(None, "env")),
        check_vma=False,
    )
```

```python
import functools
import math

import jax
import jax.numpy as jnp
from jax import lax
from jax.experimental import pallas as pl
from jax.experimental.pallas import tpu as pltpu
from jax.sharding import PartitionSpec as P

DOF = 35
HS = 2
SUB = 32
ITERS = 3
LANES = 128
WIDE = 256
VOFF = -(-DOF // 8) * 8
DEPTH = 2 * VOFF
PER = LANES // DOF
SPARE = PER * DOF

step_length = 0.05
fine_dt = step_length / SUB
TWO_PI = 2.0 * math.pi
MESH = pl.DeviceIdType.MESH
F32 = jnp.float32
BF16 = jnp.bfloat16

SIN = (
    6.2831825127387075, -41.34139305306742, 81.59546378559027,
    -76.5727543587307, 41.17302274271854, -12.2199194670916,
)


def up8(n):
    return -(-n // 8) * 8


def split(value):
    high = value.astype(BF16)
    return high, (value - high.astype(F32)).astype(BF16)


def dot(left, right):
    return jnp.dot(left, right, preferred_element_type=F32)


class Plan:
    def __init__(self, slices):
        per = PER
        order = list(range(1, slices)) + [0]
        self.groups = []
        self.where = {}
        for first in range(0, slices, per):
            members = order[first : first + per]
            base = LANES * len(self.groups)
            self.groups.append((base, members))
            for pos, n in enumerate(members):
                self.where[n] = base + pos * DOF
        self.lanes = LANES * len(self.groups)
        self.later = [g for g, (base, members) in enumerate(self.groups) if members != [0]]


class Maps:
    def __init__(self, slices):
        self.index = {(n, n): n for n in range(slices)}
        self.stage = {}
        steps = {}

        def need(first, last):
            if (first, last) in steps or first == last:
                return
            half = 1 << ((last - first).bit_length() - 1)
            need(first, first + half - 1)
            need(first + half, last)
            steps[first, last] = (half, (first, first + half - 1), (first + half, last))

        half = 1
        while half < slices:
            self.stage[half] = []
            for first in range(half, slices, 2 * half):
                for n in range(first, min(first + half, slices)):
                    need(first, n)
            half *= 2
        for key in steps:
            self.index[key] = len(self.index)
        for key, (half, left, right) in steps.items():
            self.stage[half].append((self.index[key], self.index[left], self.index[right]))
        self.count = len(self.index)


class Message:
    def __init__(self, steps, local, epd):
        self.steps, self.local, self.epd = steps, local, epd
        count = steps + local
        self.tiles = -(-count // PER)
        self.rows = []
        self.start = []
        base = 0
        for tile in range(self.tiles):
            pieces = range(tile * PER, min(count, (tile + 1) * PER))
            tall = any(i >= steps for i in pieces)
            rows = max(up8(epd), up8(DOF)) if tall else up8(epd)
            self.start.append(base)
            self.rows.append(rows)
            base += rows
        self.total = base

    def place(self, piece):
        tile, pos = divmod(piece, PER)
        return self.start[tile], pos * DOF


def kernel(
    tm, env, local, total_env,
    contact_h, torque_h, minv_h, init_h, stiff_h, damp_h, gravity_h, cstiff_h, cdamp_h,
    states_out, corr_out,
    contact, torque, minv, init, stiff_r, damp_r, gravity_r, cstiff_r, cdamp_r,
    tx, rx, row, rows, srow, sums, otx, orx, turn, mtile, own,
    tq, spring, fric, grav, cspring, cfric, wgt, wtmp, ybuf, ubuf, by, bu, ly, lu, hmap, lmap, xs,
    tsend, trecv, esend, erecv, ssend, srecv, osend, orecv, isem,
):
    slices = local * tm
    steps = local * HS
    env_local = contact.shape[1]
    epd = env_local // tm
    plan = Plan(slices)
    maps = Maps(slices)
    msg = Message(steps, local, epd)
    me_t = lax.axis_index("tm")
    me_e = lax.axis_index("env")
    barrier = pltpu.get_barrier_semaphore()

    def tm_peer(k):
        return {"tm": lax.rem(me_t + k, tm), "env": me_e}

    def env_peer(k):
        return {"tm": me_t, "env": lax.rem(me_e + k, env)}

    for k in range(1, env):
        pl.semaphore_signal(barrier, inc=1, device_id=env_peer(k), device_id_type=MESH)
    for k in range(1, tm):
        pl.semaphore_signal(barrier, inc=1, device_id=tm_peer(k), device_id_type=MESH)

    pairs = (
        (contact_h, contact), (torque_h, torque), (minv_h, minv), (init_h, init),
        (stiff_h, stiff_r), (damp_h, damp_r), (gravity_h, gravity_r),
        (cstiff_h, cstiff_r), (cdamp_h, cdamp_r),
    )
    loads = [pltpu.make_async_copy(a, b, isem.at[i]) for i, (a, b) in enumerate(pairs)]
    for c in loads:
        c.start()
    for c in loads:
        c.wait()

    hits = contact[...].astype(F32)
    row[...] = jnp.zeros(row.shape, F32)
    row[0:steps, :] = jnp.broadcast_to(jnp.sum(hits, axis=1, keepdims=True), (steps, LANES))
    for tile in range(msg.tiles):
        turn[...] = jnp.zeros(turn.shape, F32)
        mtile[...] = jnp.zeros(mtile.shape, F32)
        for pos in range(PER):
            piece = tile * PER + pos
            if piece < steps:
                turn[pos * DOF : (pos + 1) * DOF, :] = torque[:, piece, :]
            elif piece < steps + local:
                mtile[0:DOF, pos * DOF : (pos + 1) * DOF] = minv[:, piece - steps, :]
        if tile == 0:
            turn[SPARE : SPARE + steps, :] = hits
        turned = turn[...].T
        first, count = msg.start[tile], msg.rows[tile]
        tall = count > up8(epd) or any(
            steps <= i < steps + local for i in range(tile * PER, (tile + 1) * PER))
        for p in range(tm):
            chunk = turned[p * epd : (p + 1) * epd]
            if tall:
                tx[p, first : first + count, :] = mtile[0:count, :]
                tx[p, first : first + epd, :] = tx[p, first : first + epd, :] + chunk
            else:
                tx[p, first : first + epd, :] = chunk
    turn[...] = jnp.zeros(turn.shape, F32)
    turn[0:DOF, :] = init[0:DOF, :]
    turn[VOFF : VOFF + DOF, :] = init[DOF : 2 * DOF, :]
    turned = turn[...].T
    for p in range(tm):
        own[p] = turned[p * epd : (p + 1) * epd]

    pl.semaphore_wait(barrier, tm + env - 2)

    def row_copy(k):
        return pltpu.make_async_remote_copy(
            src_ref=row, dst_ref=rows.at[me_e], send_sem=esend.at[k], recv_sem=erecv.at[k],
            device_id=env_peer(k), device_id_type=MESH)

    def block_copy(k):
        return pltpu.make_async_remote_copy(
            src_ref=tx.at[lax.rem(me_t + k, tm)], dst_ref=rx.at[me_t],
            send_sem=tsend.at[k], recv_sem=trecv.at[k],
            device_id=tm_peer(k), device_id_type=MESH)

    def sum_copy(k):
        return pltpu.make_async_remote_copy(
            src_ref=srow, dst_ref=sums.at[me_t], send_sem=ssend.at[k], recv_sem=srecv.at[k],
            device_id=tm_peer(k), device_id_type=MESH)

    def out_copy(k):
        return pltpu.make_async_remote_copy(
            src_ref=otx.at[lax.rem(me_t + k, tm)], dst_ref=orx.at[me_t],
            send_sem=osend.at[k], recv_sem=orecv.at[k],
            device_id=tm_peer(k), device_id_type=MESH)

    row_copies = [row_copy(k) for k in range(1, env)]
    block_copies = [block_copy(k) for k in range(1, tm)]
    sum_copies = [sum_copy(k) for k in range(1, tm)]
    for c in row_copies + block_copies:
        c.start()
    rows[me_e] = row[...]
    rx[me_t] = tx[me_t]

    stiff, damp, gravity, cstiff, cdamp = (
        r[...] for r in (stiff_r, damp_r, gravity_r, cstiff_r, cdamp_r))
    ratio = float(SUB)
    unroll = SUB - 1 if len(plan.groups) * SUB <= 256 else 1
    to_u = TWO_PI / fine_dt
    for ref in (tq, spring, fric, grav, cspring, cfric, ybuf, ubuf, ly, lu):
        ref[...] = jnp.zeros(ref.shape, ref.dtype)
    for ref in (hmap, lmap):
        ref[:, DEPTH:, :] = jnp.zeros((maps.count, LANES - DEPTH, LANES), BF16)
    rank = lax.broadcasted_iota(jnp.int32, (DEPTH, DOF), 0)
    col = lax.broadcasted_iota(jnp.int32, (DEPTH, DOF), 1)
    for n in range(slices):
        cut = pl.ds(plan.where[n], DOF)
        grav[:, cut] = gravity
        ly[:, cut] = jnp.where(rank == col, 1.0, 0.0)
        lu[:, cut] = jnp.where(rank == col + VOFF, 1.0, 0.0)

    for c in row_copies:
        c.wait()
    srow[...] = jnp.sum(rows[...], axis=0) * (1.0 / total_env)
    for c in sum_copies:
        c.start()
    sums[me_t] = srow[...]
    for c in block_copies:
        c.wait()

    for n in range(slices):
        src, pos = divmod(n, local)
        cut = pl.ds(plan.where[n], DOF)
        for j in range(HS):
            step = pos * HS + j
            first, lane = msg.place(step)
            hit = rx[src, 0:epd, SPARE + step : SPARE + step + 1]
            tq[j, :, cut] = rx[src, first : first + epd, lane : lane + DOF]
            spring[j, :, cut] = TWO_PI * (stiff + hit * cstiff)
            fric[j, :, cut] = to_u * (damp + hit * cdamp)

    for g, (base, members) in enumerate(plan.groups):
        wtmp[...] = jnp.zeros(wtmp.shape, F32)
        for pos, n in enumerate(members):
            src, here = divmod(n, local)
            start, lane = msg.place(steps + here)
            wtmp[pl.ds(pos * DOF, DOF), pl.ds(pos * DOF, DOF)] = (
                fine_dt * fine_dt / TWO_PI
            ) * rx[src, start : start + DOF, lane : lane + DOF]
        high, low = split(wtmp[...])
        wgt[g, 0:LANES, :] = high
        wgt[g, LANES:, :] = low

    for c in sum_copies:
        c.wait()
    for n in range(slices):
        src, pos = divmod(n, local)
        cut = pl.ds(plan.where[n], DOF)
        for j in range(HS):
            step = pos * HS + j
            mean = sums[src, step : step + 1, 0:DOF]
            cspring[j, :, cut] = TWO_PI * (stiff + gravity + mean * cstiff)
            cfric[j, :, cut] = to_u * (damp + mean * cdamp)

    def once(part, g):
        return dot(jnp.concatenate([part, part], axis=1), wgt[g])

    def product(force, g):
        high, low = split(force)
        return once(high, g) + once(low, g)

    lane_of = lax.broadcasted_iota(jnp.int32, (1, LANES), 1)
    scale = jnp.where(lane_of < VOFF, TWO_PI, to_u)
    shrink = jnp.where(lane_of < VOFF, 1.0 / TWO_PI, 1.0 / to_u)

    def joined(y, u, depth):
        gap = jnp.zeros((depth, VOFF - DOF), F32)
        return jnp.concatenate(
            [y, gap, u, jnp.zeros((depth, LANES - VOFF - DOF), F32)], axis=1)

    def keep(index, value):
        high, low = split(value)
        hmap[index, 0:DEPTH, :] = high
        lmap[index, 0:DEPTH, :] = low

    def apply(high, low, index):
        weight = hmap[index]
        return dot(jnp.concatenate([high, low], axis=1),
                   jnp.concatenate([weight, weight], axis=0)) + dot(high, lmap[index])

    start = own[me_t] * shrink
    xs[0] = start
    ybuf[:, pl.ds(plan.where[0], DOF)] = start[:, 0:DOF]
    ubuf[:, pl.ds(plan.where[0], DOF)] = start[:, VOFF : VOFF + DOF]
    for g, (base, members) in enumerate(plan.groups):
        cut = pl.ds(base, LANES)
        y, u = ly[:, cut], lu[:, cut]
        b, a = ybuf[:, cut], ubuf[:, cut]
        for j in range(HS):
            force = -cspring[j, :, cut] * y - cfric[j, :, cut] * u
            u = u + ratio * product(force, g)
            y = y + ratio * u
            force = tq[j, :, cut] - cspring[j, :, cut] * b - cfric[j, :, cut] * a
            a = a + ratio * product(force, g)
            b = b + ratio * a
        ly[:, cut] = y
        lu[:, cut] = u
        by[:, cut] = b
        bu[:, cut] = a
    for n in range(slices):
        cut = pl.ds(plan.where[n], DOF)
        keep(n, joined(ly[:, cut], lu[:, cut], DEPTH))

    def sweep(ends, compose=False):
        ends = list(ends)
        half = 1
        while half < slices:
            for first in range(half, slices, 2 * half):
                high, low = split(ends[first - 1])
                for n in range(min(first + half, slices) - 1, first - 1, -1):
                    ends[n] = ends[n] + apply(high, low, maps.index[first, n])
            if compose:
                for target, left, right in maps.stage[half]:
                    keep(target, apply(hmap[left, 0:DEPTH, :], lmap[left, 0:DEPTH, :], right))
            half *= 2
        return ends

    def packed(yref, uref, n):
        cut = pl.ds(plan.where[n], DOF)
        return joined(yref[:, cut], uref[:, cut], epd)

    ends = sweep([packed(by, bu, n) for n in range(slices)], True)
    for n in range(slices):
        xs[n + 1] = ends[n]

    def iteration(k, corrections, active, sliced):
        for n in sliced:
            cut = pl.ds(plan.where[n], DOF)
            ybuf[:, cut] = xs[n, :, 0:DOF]
            ubuf[:, cut] = xs[n, :, VOFF : VOFF + DOF]
        carry = []
        for g in active:
            cut = pl.ds(plan.groups[g][0], LANES)
            y = ybuf[:, cut]
            carry.append((y, ubuf[:, cut], y - jnp.round(y), jnp.zeros_like(y)))
        carry = tuple(carry)

        def horizon(j, carry):
            def substep(flush, counter, carry):
                result = []
                for g, (y, u, t, rest) in zip(active, carry):
                    cut = pl.ds(plan.groups[g][0], LANES)
                    ahead = y + u
                    base = ahead - jnp.round(ahead)
                    s = t * t
                    s2 = s * s
                    poly = (SIN[5] * s + SIN[4]) * s2 + (SIN[3] * s + SIN[2])
                    poly = poly * s2 + (SIN[1] * s + SIN[0])
                    linear = ((tq[j, :, cut] + rest) - spring[j, :, cut] * y) - fric[j, :, cut] * u
                    force = linear - (grav[:, cut] * t) * poly
                    sent = force.astype(BF16)
                    rest = force - sent.astype(F32)
                    push = once(sent, g)
                    if flush:
                        push = push + once(rest.astype(BF16), g)
                        rest = jnp.zeros_like(rest)
                    result.append((ahead + push, u + push, base + push, rest))
                return tuple(result)

            carry = lax.fori_loop(0, SUB - 1, functools.partial(substep, False), carry, unroll=unroll)
            return substep(True, SUB - 1, carry)

        carry = lax.fori_loop(0, HS, horizon, carry)
        for g, (y, u, t, rest) in zip(active, carry):
            cut = pl.ds(plan.groups[g][0], LANES)
            ybuf[:, cut] = y
            ubuf[:, cut] = u
        worst = jnp.zeros((epd, 1), F32)
        moved = [packed(ybuf, ubuf, n) - xs[n + 1] if n in sliced else None for n in range(slices)]
        if moved[0] is None:
            moved[0] = jnp.zeros((epd, LANES), F32)
        changes = sweep(moved, None)
        for n in range(slices):
            real = changes[n] * scale
            worst = jnp.maximum(worst, jnp.sum(real * real, axis=1, keepdims=True))
            xs[n + 1] = xs[n + 1] + changes[n]
        return jnp.where(lane_of == DOF + k, jnp.sqrt(worst), corrections)

    groups = range(len(plan.groups))
    corrections = iteration(0, jnp.zeros((epd, LANES), F32), groups, range(slices))
    live = [n for g in plan.later for n in plan.groups[g][1]]
    corrections = lax.fori_loop(
        1, ITERS, lambda k, kept: iteration(k, kept, plan.later, live), corrections)

    span = local * epd
    for t in range(tm):
        parts = [xs[t * local + pos + 1] * scale for pos in range(local)]
        parts[0] = parts[0] + corrections
        turned = jnp.concatenate(parts, axis=0).T
        otx[t, :, 0:span] = turned[0:VOFF]
        otx[t, :, span : 2 * span] = turned[VOFF:DEPTH]
    out_copies = [out_copy(k) for k in range(1, tm)]
    for c in out_copies:
        c.start()
    orx[me_t] = otx[me_t]
    for c in out_copies:
        c.wait()

    across = LANES // epd
    lanes = lax.broadcasted_iota(jnp.int32, (VOFF, LANES), 1)
    for part in range(2):
        for pos in range(local):
            off = part * span + pos * epd
            for tile in range(env_local // LANES):
                acc = None
                for q in range(across):
                    block_in = orx[tile * across + q]
                    shift = (q * epd - off) % LANES
                    moved = pltpu.roll(block_in, shift, 1) if shift else block_in
                    acc = moved if acc is None else jnp.where(lanes >= q * epd, moved, acc)
                cut = pl.ds(tile * LANES, LANES)
                states_out[part * DOF : (part + 1) * DOF, pos, cut] = acc[0:DOF]
                if part == 0 and pos == 0:
                    corr_out[:, cut] = acc[DOF : DOF + ITERS]


def body(tm, env, init_state, torque, contact, mass_inverse, stiffness, damping, gravity,
         contact_stiffness, contact_damping):
    local = mass_inverse.shape[0]
    env_local = init_state.shape[1]
    epd = env_local // tm
    steps = local * HS
    slices = local * tm
    plan = Plan(slices)
    maps = Maps(slices).count
    msg = Message(steps, local, epd)
    vmem = pl.BlockSpec(memory_space=pltpu.VMEM)
    dma = pltpu.SemaphoreType.DMA
    prm = [p.reshape(1, DOF) for p in (stiffness, damping, gravity, contact_stiffness, contact_damping)]
    lanes = plan.lanes
    groups = len(plan.groups)
    big = pltpu.VMEM((epd, lanes), F32)
    both = pltpu.VMEM((HS, epd, lanes), F32)
    thin = pltpu.VMEM((HS, 1, lanes), F32)
    row = (up8(steps), LANES)
    states, corrections = pl.pallas_call(
        functools.partial(kernel, tm, env, local, env_local * env),
        out_shape=(
            pltpu.VMEM((2 * DOF, local, env_local), F32),
            pltpu.VMEM((ITERS, env_local), F32),
        ),
        in_specs=[pl.BlockSpec(memory_space=pl.ANY)] * 9,
        out_specs=(vmem, vmem),
        scratch_shapes=[
            pltpu.VMEM((steps, env_local), jnp.int32),
            pltpu.VMEM((DOF, steps, env_local), F32),
            pltpu.VMEM((DOF, local, DOF), F32),
            pltpu.VMEM((2 * DOF, env_local), F32),
        ] + [pltpu.VMEM((1, DOF), F32)] * 5 + [
            pltpu.VMEM((tm, msg.total, LANES), F32), pltpu.VMEM((tm, msg.total, LANES), F32),
            pltpu.VMEM(row, F32), pltpu.VMEM((env,) + row, F32),
            pltpu.VMEM(row, F32), pltpu.VMEM((tm,) + row, F32),
            pltpu.VMEM((tm, VOFF, LANES), F32), pltpu.VMEM((tm, VOFF, LANES), F32),
            pltpu.VMEM((LANES, env_local), F32),
            pltpu.VMEM((max(msg.rows), LANES), F32),
            pltpu.VMEM((tm, epd, LANES), F32),
            both, both, both, pltpu.VMEM((1, lanes), F32), thin, thin,
            pltpu.VMEM((groups, WIDE, LANES), BF16),
            pltpu.VMEM((LANES, LANES), F32),
            big, big, big, big,
            pltpu.VMEM((DEPTH, lanes), F32), pltpu.VMEM((DEPTH, lanes), F32),
            pltpu.VMEM((maps, LANES, LANES), BF16), pltpu.VMEM((maps, LANES, LANES), BF16),
            pltpu.VMEM((slices + 1, epd, LANES), F32),
            dma((tm,)), dma((tm,)), dma((env,)), dma((env,)),
            dma((tm,)), dma((tm,)), dma((tm,)), dma((tm,)), dma((9,)),
        ],
        compiler_params=pltpu.CompilerParams(collective_id=0, has_side_effects=True),
        name="parareal",
    )(contact, jnp.transpose(torque, (1, 0, 2)),
      jnp.transpose(mass_inverse, (1, 0, 2)), init_state, *prm)
    return jnp.transpose(states, (1, 0, 2)), corrections


def solution(mesh):
    placed = (
        P(None, "env"),
        P("tm", None, "env"),
        P("tm", "env"),
        P("tm", None, None),
        P(),
        P(),
        P(),
        P(),
        P(),
    )
    return jax.shard_map(
        functools.partial(body, mesh.shape["tm"], mesh.shape["env"]),
        mesh=mesh,
        in_specs=placed,
        out_specs=(P("tm", None, "env"), P(None, "env")),
        check_vma=False,
    )
```

```python
import functools
import math

import jax
import jax.numpy as jnp
from jax import lax
from jax.experimental import pallas as pl
from jax.experimental.pallas import tpu as pltpu
from jax.sharding import PartitionSpec as P

DOF = 35
HS = 2
SUB = 32
ITERS = 3
LANES = 128
WIDE = 256
VOFF = -(-DOF // 8) * 8
DEPTH = 2 * VOFF
PER = LANES // DOF
SPARE = PER * DOF

step_length = 0.05
fine_dt = step_length / SUB
TWO_PI = 2.0 * math.pi
MESH = pl.DeviceIdType.MESH
F32 = jnp.float32
BF16 = jnp.bfloat16

SIN = (
    6.2831825127387075, -41.34139305306742, 81.59546378559027,
    -76.5727543587307, 41.17302274271854, -12.2199194670916,
)


def up8(n):
    return -(-n // 8) * 8


def split(value):
    high = value.astype(BF16)
    return high, (value - high.astype(F32)).astype(BF16)


def dot(left, right):
    return jnp.dot(left, right, preferred_element_type=F32)


class Plan:
    def __init__(self, slices):
        per = PER
        order = list(range(1, slices)) + [0]
        self.groups = []
        self.where = {}
        for first in range(0, slices, per):
            members = order[first : first + per]
            base = LANES * len(self.groups)
            self.groups.append((base, members))
            for pos, n in enumerate(members):
                self.where[n] = base + pos * DOF
        self.lanes = LANES * len(self.groups)
        self.later = [g for g, (base, members) in enumerate(self.groups) if members != [0]]


class Maps:
    def __init__(self, slices):
        self.index = {(n, n): n for n in range(slices)}
        self.stage = {}
        steps = {}

        def need(first, last):
            if (first, last) in steps or first == last:
                return
            half = 1 << ((last - first).bit_length() - 1)
            need(first, first + half - 1)
            need(first + half, last)
            steps[first, last] = (half, (first, first + half - 1), (first + half, last))

        half = 1
        while half < slices:
            self.stage[half] = []
            for first in range(half, slices, 2 * half):
                for n in range(first, min(first + half, slices)):
                    need(first, n)
            half *= 2
        for key in steps:
            self.index[key] = len(self.index)
        for key, (half, left, right) in steps.items():
            self.stage[half].append((self.index[key], self.index[left], self.index[right]))
        self.count = len(self.index)


class Message:
    def __init__(self, steps, local, epd):
        self.steps, self.local, self.epd = steps, local, epd
        count = steps + local
        self.tiles = -(-count // PER)
        self.rows = []
        self.start = []
        base = 0
        for tile in range(self.tiles):
            pieces = range(tile * PER, min(count, (tile + 1) * PER))
            tall = any(i >= steps for i in pieces)
            rows = max(up8(epd), up8(DOF)) if tall else up8(epd)
            self.start.append(base)
            self.rows.append(rows)
            base += rows
        self.total = base

    def place(self, piece):
        tile, pos = divmod(piece, PER)
        return self.start[tile], pos * DOF


def kernel(
    tm, env, local, total_env,
    contact_h, torque_h, minv_h, init_h, stiff_h, damp_h, gravity_h, cstiff_h, cdamp_h,
    states_out, corr_out,
    contact, torque, minv, init, stiff_r, damp_r, gravity_r, cstiff_r, cdamp_r,
    tx, rx, row, rows, srow, sums, otx, orx, turn, mtile, own,
    tq, spring, fric, prow, cspring, cfric, wgt, wtmp, ybuf, ubuf, by, bu, ly, lu, maps_w, xs,
    tsem, esem, ssem, osem, isem,
):
    slices = local * tm
    steps = local * HS
    env_local = contact.shape[1]
    epd = env_local // tm
    plan = Plan(slices)
    maps = Maps(slices)
    msg = Message(steps, local, epd)
    me_t = lax.axis_index("tm")
    me_e = lax.axis_index("env")
    barrier = pltpu.get_barrier_semaphore()

    def tm_peer(k):
        return {"tm": lax.rem(me_t + k, tm), "env": me_e}

    def env_peer(k):
        return {"tm": me_t, "env": lax.rem(me_e + k, env)}

    for k in range(1, env):
        pl.semaphore_signal(barrier, inc=1, device_id=env_peer(k), device_id_type=MESH)
    for k in range(1, tm):
        pl.semaphore_signal(barrier, inc=1, device_id=tm_peer(k), device_id_type=MESH)

    pairs = (
        (contact_h, contact), (torque_h, torque), (minv_h, minv), (init_h, init),
        (stiff_h, stiff_r), (damp_h, damp_r), (gravity_h, gravity_r),
        (cstiff_h, cstiff_r), (cdamp_h, cdamp_r),
    )
    loads = [pltpu.make_async_copy(a, b, isem.at[i]) for i, (a, b) in enumerate(pairs)]
    for c in loads:
        c.start()
    loads[0].wait()
    hits = contact[...].astype(F32)
    row[...] = jnp.zeros(row.shape, F32)
    row[0:steps, :] = jnp.broadcast_to(jnp.sum(hits, axis=1, keepdims=True), (steps, LANES))
    for c in loads[1:3]:
        c.wait()

    for tile in range(msg.tiles):
        turn[...] = jnp.zeros(turn.shape, F32)
        mtile[...] = jnp.zeros(mtile.shape, F32)
        for pos in range(PER):
            piece = tile * PER + pos
            if piece < steps:
                turn[pos * DOF : (pos + 1) * DOF, :] = torque[:, piece, :]
            elif piece < steps + local:
                mtile[0:DOF, pos * DOF : (pos + 1) * DOF] = minv[:, piece - steps, :]
        if tile == 0:
            turn[SPARE : SPARE + steps, :] = hits
        turned = turn[...].T
        first, count = msg.start[tile], msg.rows[tile]
        tall = count > up8(epd) or any(
            steps <= i < steps + local for i in range(tile * PER, (tile + 1) * PER))
        for p in range(tm):
            chunk = turned[p * epd : (p + 1) * epd]
            if tall:
                tx[p, first : first + count, :] = mtile[0:count, :]
                tx[p, first : first + epd, :] = tx[p, first : first + epd, :] + chunk
            else:
                tx[p, first : first + epd, :] = chunk

    pl.semaphore_wait(barrier, tm + env - 2)

    def sends(src, dst, sem, count, peer):
        return [
            pltpu.make_async_remote_copy(
                src_ref=src(k), dst_ref=dst, send_sem=sem.at[0], recv_sem=sem.at[1],
                device_id=peer(k), device_id_type=MESH)
            for k in range(1, count)
        ]

    def finish(src, dst, sem, peer):
        all_of = pltpu.make_async_remote_copy(
            src_ref=src, dst_ref=dst, send_sem=sem.at[0], recv_sem=sem.at[1],
            device_id=peer(1), device_id_type=MESH)
        all_of.wait_send()
        all_of.wait_recv()

    def to_peer(ref):
        return lambda k: ref.at[lax.rem(me_t + k, tm)]

    most, few = pl.ds(0, tm - 1), pl.ds(0, env - 1)
    for c in sends(lambda k: row, rows.at[me_e], esem, env, env_peer):
        c.start()
    for c in sends(to_peer(tx), rx.at[me_t], tsem, tm, tm_peer):
        c.start()
    for c in loads[3:]:
        c.wait()
    turn[...] = jnp.zeros(turn.shape, F32)
    turn[0:DOF, :] = init[0:DOF, :]
    turn[VOFF : VOFF + DOF, :] = init[DOF : 2 * DOF, :]
    turned = turn[...].T
    for p in range(tm):
        own[p] = turned[p * epd : (p + 1) * epd]
    rows[me_e] = row[...]
    rx[me_t] = tx[me_t]

    ratio = float(SUB)
    to_u = TWO_PI / fine_dt
    high_rows = up8(epd)
    lane_of = lax.broadcasted_iota(jnp.int32, (1, LANES), 1)
    wide_lane = lax.broadcasted_iota(jnp.int32, (high_rows, LANES), 1)

    prow[...] = jnp.zeros(prow.shape, F32)
    for i, ref in enumerate((stiff_r, damp_r, gravity_r, cstiff_r, cdamp_r)):
        for pos in range(PER):
            prow[i : i + 1, pos * DOF : (pos + 1) * DOF] = ref[...]
    stiff, damp, gravity, cstiff, cdamp = (prow[i : i + 1, :] for i in range(5))
    for ref in (ybuf, ubuf, ly, lu):
        ref[...] = jnp.zeros(ref.shape, ref.dtype)
    maps_w[:, 3 * DEPTH :, :] = jnp.zeros((maps.count, WIDE - 3 * DEPTH, LANES), BF16)
    rank = lax.broadcasted_iota(jnp.int32, (DEPTH, DOF), 0)
    col = lax.broadcasted_iota(jnp.int32, (DEPTH, DOF), 1)
    for n in range(slices):
        span_n = pl.ds(plan.where[n], DOF)
        ly[:, span_n] = jnp.where(rank == col, 1.0, 0.0)
        lu[:, span_n] = jnp.where(rank == col + VOFF, 1.0, 0.0)

    finish(rows.at[few], rows.at[few], esem, env_peer)
    srow[...] = jnp.sum(rows[...], axis=0) * (1.0 / total_env)
    for c in sends(lambda k: srow, sums.at[me_t], ssem, tm, tm_peer):
        c.start()
    sums[me_t] = srow[...]
    finish(tx.at[most], rx.at[most], tsem, tm_peer)

    def by_lane(values, lanes):
        out = values[0]
        for pos in range(1, len(values)):
            out = jnp.where(lanes >= pos * DOF, values[pos], out)
        return out

    def moved_to(value, shift):
        shift = shift % LANES
        return pltpu.roll(value, shift, 1) if shift else value

    for g, (base, members) in enumerate(plan.groups):
        span_g = pl.ds(base, LANES)
        for j in range(HS):
            force, hit = [], []
            for pos, n in enumerate(members):
                src, here = divmod(n, local)
                step = here * HS + j
                first, lane = msg.place(step)
                piece = rx[src, first : first + high_rows, :]
                force.append(moved_to(piece, pos * DOF - lane))
                flag = rx[src, 0:high_rows, SPARE + step : SPARE + step + 1]
                hit.append(jnp.broadcast_to(flag, (high_rows, LANES)))
            touch = by_lane(hit, wide_lane)[0:epd]
            tq[j, :, span_g] = by_lane(force, wide_lane)[0:epd]
            spring[j, :, span_g] = TWO_PI * stiff + touch * (TWO_PI * cstiff)
            fric[j, :, span_g] = to_u * damp + touch * (to_u * cdamp)

    tall_lane = lax.broadcasted_iota(jnp.int32, (VOFF, LANES), 1)
    for g, (base, members) in enumerate(plan.groups):
        wtmp[...] = jnp.zeros(wtmp.shape, F32)
        for pos, n in enumerate(members):
            src, here = divmod(n, local)
            first, lane = msg.place(steps + here)
            piece = moved_to(rx[src, first : first + VOFF, :], pos * DOF - lane)
            inside = (tall_lane >= pos * DOF) & (tall_lane < (pos + 1) * DOF)
            piece = jnp.where(inside, (fine_dt * fine_dt / TWO_PI) * piece, 0.0)
            wtmp[pl.ds(pos * DOF, DOF), :] = piece[0:DOF]
        high, low = split(wtmp[...])
        wgt[g, 0:LANES, :] = high
        wgt[g, LANES:, :] = low

    finish(sums.at[most], sums.at[most], ssem, tm_peer)
    for g, (base, members) in enumerate(plan.groups):
        span_g = pl.ds(base, LANES)
        for j in range(HS):
            means = []
            for n in members:
                src, here = divmod(n, local)
                step = here * HS + j
                means.append(sums[src, step : step + 1, :])
            mean = by_lane(means, lane_of)
            cspring[j, :, span_g] = TWO_PI * (stiff + gravity + mean * cstiff)
            cfric[j, :, span_g] = to_u * (damp + mean * cdamp)

    def once(part, g):
        return dot(jnp.concatenate([part, part], axis=1), wgt[g])

    def product(force, g):
        high, low = split(force)
        return once(high, g) + once(low, g)

    scale = jnp.where(lane_of < VOFF, TWO_PI, to_u)
    shrink = jnp.where(lane_of < VOFF, 1.0 / TWO_PI, 1.0 / to_u)

    def joined(y, u, depth):
        gap = jnp.zeros((depth, VOFF - DOF), F32)
        return jnp.concatenate(
            [y, gap, u, jnp.zeros((depth, LANES - VOFF - DOF), F32)], axis=1)

    spill = 2 * DEPTH - LANES

    def spread(value):
        lanes = lax.broadcasted_iota(jnp.int32, value.shape, 1)
        high = value.astype(BF16).astype(F32)
        low = moved_to(value - high, DEPTH)
        left = jnp.where(lanes < DEPTH, high, low)
        right = jnp.where(lanes < spill, low, moved_to(high, spill))
        return jnp.concatenate([left, right], axis=1).astype(BF16)

    values = {}

    def keep(index, value):
        values[index] = value
        high, low = split(value)
        maps_w[index, 0:DEPTH, :] = high
        maps_w[index, DEPTH : 2 * DEPTH, :] = high
        maps_w[index, 2 * DEPTH : 3 * DEPTH, :] = low

    def apply(left, index):
        return dot(left, maps_w[index])

    start = own[me_t] * shrink
    xs[0] = start
    ybuf[:, pl.ds(plan.where[0], DOF)] = start[:, 0:DOF]
    ubuf[:, pl.ds(plan.where[0], DOF)] = start[:, VOFF : VOFF + DOF]
    spans = [pl.ds(base, LANES) for base, members in plan.groups]
    every = range(len(spans))
    y, u = [ly[:, c] for c in spans], [lu[:, c] for c in spans]
    b, a = [ybuf[:, c] for c in spans], [ubuf[:, c] for c in spans]
    for j in range(HS):
        for g in every:
            c = spans[g]
            force = tq[j, :, c] - cspring[j, :, c] * b[g] - cfric[j, :, c] * a[g]
            a[g] = a[g] + ratio * product(force, g)
            force = -cspring[j, :, c] * y[g] - cfric[j, :, c] * u[g]
            u[g] = u[g] + ratio * product(force, g)
        for g in every:
            b[g] = b[g] + ratio * a[g]
            y[g] = y[g] + ratio * u[g]
    for g in every:
        ly[:, spans[g]], lu[:, spans[g]] = y[g], u[g]
        by[:, spans[g]], bu[:, spans[g]] = b[g], a[g]
    for n in range(slices):
        cut = pl.ds(plan.where[n], DOF)
        keep(n, joined(ly[:, cut], lu[:, cut], DEPTH))

    def sweep(ends, compose=False):
        ends = list(ends)
        half = 1
        while half < slices:
            for first in range(half, slices, 2 * half):
                left = spread(ends[first - 1])
                for n in range(min(first + half, slices) - 1, first - 1, -1):
                    ends[n] = ends[n] + apply(left, maps.index[first, n])
            if compose:
                for target, left, right in maps.stage[half]:
                    keep(target, apply(spread(values[left]), right))
            half *= 2
        return ends

    def packed(yref, uref, n):
        cut = pl.ds(plan.where[n], DOF)
        return joined(yref[:, cut], uref[:, cut], epd)

    ends = sweep([packed(by, bu, n) for n in range(slices)], True)
    for n in range(slices):
        xs[n + 1] = ends[n]

    unroll = SUB - 1 if len(plan.groups) * SUB <= 256 else 1
    grav = gravity

    def iteration(k, corrections, active, sliced):
        for n in sliced:
            cut = pl.ds(plan.where[n], DOF)
            ybuf[:, cut] = xs[n, :, 0:DOF]
            ubuf[:, cut] = xs[n, :, VOFF : VOFF + DOF]
        carry = []
        for g in active:
            cut = pl.ds(plan.groups[g][0], LANES)
            y = ybuf[:, cut]
            carry.append((y, ubuf[:, cut], y - jnp.round(y), jnp.zeros_like(y)))
        carry = tuple(carry)

        def horizon(j, carry):
            def substep(flush, counter, carry):
                result = []
                for g, (y, u, t, rest) in zip(active, carry):
                    cut = pl.ds(plan.groups[g][0], LANES)
                    ahead = y + u
                    base = ahead - jnp.round(ahead)
                    s = t * t
                    s2 = s * s
                    weight = grav * t
                    weight2 = weight * s2
                    linear = ((tq[j, :, cut] + rest) - spring[j, :, cut] * y) - fric[j, :, cut] * u
                    force = linear - weight * (SIN[1] * s + SIN[0])
                    force = force - weight2 * (SIN[3] * s + SIN[2])
                    force = force - (weight2 * s2) * (SIN[5] * s + SIN[4])
                    sent = force.astype(BF16)
                    rest = force - sent.astype(F32)
                    push = once(sent, g)
                    if flush:
                        push = push + once(rest.astype(BF16), g)
                        rest = jnp.zeros_like(rest)
                    result.append((ahead + push, u + push, base + push, rest))
                return tuple(result)

            carry = lax.fori_loop(0, SUB - 1, functools.partial(substep, False), carry, unroll=unroll)
            return substep(True, SUB - 1, carry)

        if unroll > 1:
            for j in range(HS):
                carry = horizon(j, carry)
        else:
            carry = lax.fori_loop(0, HS, horizon, carry)
        for g, (y, u, t, rest) in zip(active, carry):
            cut = pl.ds(plan.groups[g][0], LANES)
            ybuf[:, cut] = y
            ubuf[:, cut] = u
        worst = jnp.zeros((epd, 1), F32)
        moved = [packed(ybuf, ubuf, n) - xs[n + 1] if n in sliced else None for n in range(slices)]
        if moved[0] is None:
            moved[0] = jnp.zeros((epd, LANES), F32)
        changes = sweep(moved, None)
        for n in range(slices):
            real = changes[n] * scale
            worst = jnp.maximum(worst, jnp.sum(real * real, axis=1, keepdims=True))
            xs[n + 1] = xs[n + 1] + changes[n]
        return jnp.where(lane_of == DOF + k, jnp.sqrt(worst), corrections)

    groups = range(len(plan.groups))
    corrections = iteration(0, jnp.zeros((epd, LANES), F32), groups, range(slices))
    live = [n for g in plan.later for n in plan.groups[g][1]]
    corrections = lax.fori_loop(
        1, ITERS, lambda k, kept: iteration(k, kept, plan.later, live), corrections)

    span = local * epd
    for t in range(tm):
        parts = [xs[t * local + pos + 1] * scale for pos in range(local)]
        parts[0] = parts[0] + corrections
        turned = jnp.concatenate(parts, axis=0).T
        otx[t, :, 0:span] = turned[0:VOFF]
        otx[t, :, span : 2 * span] = turned[VOFF:DEPTH]
    for c in sends(to_peer(otx), orx.at[me_t], osem, tm, tm_peer):
        c.start()
    orx[me_t] = otx[me_t]
    finish(otx.at[most], orx.at[most], osem, tm_peer)

    across = LANES // epd
    lanes = lax.broadcasted_iota(jnp.int32, (VOFF, LANES), 1)
    for part in range(2):
        for pos in range(local):
            off = part * span + pos * epd
            for tile in range(env_local // LANES):
                acc = None
                for q in range(across):
                    block_in = orx[tile * across + q]
                    shift = (q * epd - off) % LANES
                    moved = pltpu.roll(block_in, shift, 1) if shift else block_in
                    acc = moved if acc is None else jnp.where(lanes >= q * epd, moved, acc)
                cut = pl.ds(tile * LANES, LANES)
                states_out[part * DOF : (part + 1) * DOF, pos, cut] = acc[0:DOF]
                if part == 0 and pos == 0:
                    corr_out[:, cut] = acc[DOF : DOF + ITERS]


def body(tm, env, init_state, torque, contact, mass_inverse, stiffness, damping, gravity,
         contact_stiffness, contact_damping):
    local = mass_inverse.shape[0]
    env_local = init_state.shape[1]
    epd = env_local // tm
    steps = local * HS
    slices = local * tm
    plan = Plan(slices)
    maps = Maps(slices).count
    msg = Message(steps, local, epd)
    vmem = pl.BlockSpec(memory_space=pltpu.VMEM)
    dma = pltpu.SemaphoreType.DMA
    prm = [p.reshape(1, DOF) for p in (stiffness, damping, gravity, contact_stiffness, contact_damping)]
    lanes = plan.lanes
    groups = len(plan.groups)
    big = pltpu.VMEM((epd, lanes), F32)
    both = pltpu.VMEM((HS, epd, lanes), F32)
    thin = pltpu.VMEM((HS, 1, lanes), F32)
    row = (up8(steps), LANES)
    states, corrections = pl.pallas_call(
        functools.partial(kernel, tm, env, local, env_local * env),
        out_shape=(
            pltpu.VMEM((2 * DOF, local, env_local), F32),
            pltpu.VMEM((ITERS, env_local), F32),
        ),
        in_specs=[pl.BlockSpec(memory_space=pl.ANY)] * 9,
        out_specs=(vmem, vmem),
        scratch_shapes=[
            pltpu.VMEM((steps, env_local), jnp.int32),
            pltpu.VMEM((DOF, steps, env_local), F32),
            pltpu.VMEM((DOF, local, DOF), F32),
            pltpu.VMEM((2 * DOF, env_local), F32),
        ] + [pltpu.VMEM((1, DOF), F32)] * 5 + [
            pltpu.VMEM((tm, msg.total, LANES), F32), pltpu.VMEM((tm, msg.total, LANES), F32),
            pltpu.VMEM(row, F32), pltpu.VMEM((env,) + row, F32),
            pltpu.VMEM(row, F32), pltpu.VMEM((tm,) + row, F32),
            pltpu.VMEM((tm, VOFF, LANES), F32), pltpu.VMEM((tm, VOFF, LANES), F32),
            pltpu.VMEM((LANES, env_local), F32),
            pltpu.VMEM((max(msg.rows), LANES), F32),
            pltpu.VMEM((tm, epd, LANES), F32),
            both, both, both, pltpu.VMEM((8, LANES), F32), thin, thin,
            pltpu.VMEM((groups, WIDE, LANES), BF16),
            pltpu.VMEM((LANES, LANES), F32),
            big, big, big, big,
            pltpu.VMEM((DEPTH, lanes), F32), pltpu.VMEM((DEPTH, lanes), F32),
            pltpu.VMEM((maps, WIDE, LANES), BF16),
            pltpu.VMEM((slices + 1, epd, LANES), F32),
            dma((2,)), dma((2,)), dma((2,)), dma((2,)), dma((9,)),
        ],
        compiler_params=pltpu.CompilerParams(collective_id=0, has_side_effects=True),
        name="parareal",
    )(contact, jnp.transpose(torque, (1, 0, 2)),
      jnp.transpose(mass_inverse, (1, 0, 2)), init_state, *prm)
    return jnp.transpose(states, (1, 0, 2)), corrections


def solution(mesh):
    placed = (
        P(None, "env"),
        P("tm", None, "env"),
        P("tm", "env"),
        P("tm", None, None),
        P(),
        P(),
        P(),
        P(),
        P(),
    )
    return jax.shard_map(
        functools.partial(body, mesh.shape["tm"], mesh.shape["env"]),
        mesh=mesh,
        in_specs=placed,
        out_specs=(P("tm", None, "env"), P(None, "env")),
        check_vma=False,
    )
```

```python
import functools
import math

import jax
import jax.numpy as jnp
from jax import lax
from jax.experimental import pallas as pl
from jax.experimental.pallas import tpu as pltpu
from jax.sharding import PartitionSpec as P

DOF = 35
HS = 2
SUB = 32
ITERS = 3
LANES = 128
WIDE = 256
VOFF = -(-DOF // 8) * 8
DEPTH = 2 * VOFF
PER = LANES // DOF
SPARE = PER * DOF

step_length = 0.05
fine_dt = step_length / SUB
TWO_PI = 2.0 * math.pi
MESH = pl.DeviceIdType.MESH
F32 = jnp.float32
BF16 = jnp.bfloat16

SIN = (
    6.2831825127387075, -41.34139305306742, 81.59546378559027,
    -76.5727543587307, 41.17302274271854, -12.2199194670916,
)


def up8(n):
    return -(-n // 8) * 8


def split(value):
    high = value.astype(BF16)
    return high, (value - high.astype(F32)).astype(BF16)


def dot(left, right):
    return jnp.dot(left, right, preferred_element_type=F32)


class Plan:
    def __init__(self, slices):
        per = PER
        order = list(range(1, slices)) + [0]
        self.groups = []
        self.where = {}
        for first in range(0, slices, per):
            members = order[first : first + per]
            base = LANES * len(self.groups)
            self.groups.append((base, members))
            for pos, n in enumerate(members):
                self.where[n] = base + pos * DOF
        self.lanes = LANES * len(self.groups)
        self.later = [g for g, (base, members) in enumerate(self.groups) if members != [0]]


class Maps:
    def __init__(self, slices):
        self.index = {(n, n): n for n in range(slices)}
        self.stage = {}
        steps = {}

        def need(first, last):
            if (first, last) in steps or first == last:
                return
            half = 1 << ((last - first).bit_length() - 1)
            need(first, first + half - 1)
            need(first + half, last)
            steps[first, last] = (half, (first, first + half - 1), (first + half, last))

        half = 1
        while half < slices:
            self.stage[half] = []
            for first in range(half, slices, 2 * half):
                for n in range(first, min(first + half, slices)):
                    need(first, n)
            half *= 2
        for key in steps:
            self.index[key] = len(self.index)
        for key, (half, left, right) in steps.items():
            self.stage[half].append((self.index[key], self.index[left], self.index[right]))
        self.count = len(self.index)
        self.after = {
            (half, right): (target, left)
            for half, stage in self.stage.items() for target, left, right in stage
        }


class Message:
    def __init__(self, steps, local, epd):
        self.steps, self.local, self.epd = steps, local, epd
        count = steps + local
        self.tiles = -(-count // PER)
        self.rows = []
        self.start = []
        base = 0
        for tile in range(self.tiles):
            pieces = range(tile * PER, min(count, (tile + 1) * PER))
            tall = any(i >= steps for i in pieces)
            rows = max(up8(epd), up8(DOF)) if tall else up8(epd)
            self.start.append(base)
            self.rows.append(rows)
            base += rows
        self.total = base

    def place(self, piece):
        tile, pos = divmod(piece, PER)
        return self.start[tile], pos * DOF


def kernel(
    tm, env, local, total_env,
    contact_h, torque_h, minv_h, init_h, stiff_h, damp_h, gravity_h, cstiff_h, cdamp_h,
    states_out, corr_out,
    contact, torque, minv, init, stiff_r, damp_r, gravity_r, cstiff_r, cdamp_r,
    tx, rx, row, rows, srow, sums, otx, orx, turn, mtile, own,
    tq, spring, fric, prow, cspring, cfric, wgt, wtmp, ybuf, ubuf, by, bu, ly, lu, maps_w, xs,
    tsem, esem, ssem, osem, csem, isem, delta, corr_t, ctx, crx,
):
    slices = local * tm
    steps = local * HS
    env_local = contact.shape[1]
    epd = env_local // tm
    plan = Plan(slices)
    maps = Maps(slices)
    msg = Message(steps, local, epd)
    me_t = lax.axis_index("tm")
    me_e = lax.axis_index("env")
    barrier = pltpu.get_barrier_semaphore()

    def tm_peer(k):
        return {"tm": lax.rem(me_t + k, tm), "env": me_e}

    def env_peer(k):
        return {"tm": me_t, "env": lax.rem(me_e + k, env)}

    for k in range(1, env):
        pl.semaphore_signal(barrier, inc=1, device_id=env_peer(k), device_id_type=MESH)
    for k in range(1, tm):
        pl.semaphore_signal(barrier, inc=1, device_id=tm_peer(k), device_id_type=MESH)

    pairs = (
        (contact_h, contact), (torque_h, torque), (minv_h, minv), (init_h, init),
        (stiff_h, stiff_r), (damp_h, damp_r), (gravity_h, gravity_r),
        (cstiff_h, cstiff_r), (cdamp_h, cdamp_r),
    )
    loads = [pltpu.make_async_copy(a, b, isem.at[i]) for i, (a, b) in enumerate(pairs)]
    for c in loads:
        c.start()
    loads[0].wait()
    hits = contact[...].astype(F32)
    row[...] = jnp.zeros(row.shape, F32)
    row[0:steps, :] = jnp.broadcast_to(jnp.sum(hits, axis=1, keepdims=True), (steps, LANES))
    for c in loads[1:3]:
        c.wait()

    for tile in range(msg.tiles):
        turn[...] = jnp.zeros(turn.shape, F32)
        mtile[...] = jnp.zeros(mtile.shape, F32)
        for pos in range(PER):
            piece = tile * PER + pos
            if piece < steps:
                turn[pos * DOF : (pos + 1) * DOF, :] = torque[:, piece, :]
            elif piece < steps + local:
                mtile[0:DOF, pos * DOF : (pos + 1) * DOF] = minv[:, piece - steps, :]
        if tile == 0:
            turn[SPARE : SPARE + steps, :] = hits
        turned = turn[...].T
        first, count = msg.start[tile], msg.rows[tile]
        tall = count > up8(epd) or any(
            steps <= i < steps + local for i in range(tile * PER, (tile + 1) * PER))
        for p in range(tm):
            chunk = turned[p * epd : (p + 1) * epd]
            if tall:
                tx[p, first : first + count, :] = mtile[0:count, :]
                tx[p, first : first + epd, :] = tx[p, first : first + epd, :] + chunk
            else:
                tx[p, first : first + epd, :] = chunk

    pl.semaphore_wait(barrier, tm + env - 2)

    def sends(src, dst, sem, count, peer):
        return [
            pltpu.make_async_remote_copy(
                src_ref=src(k), dst_ref=dst, send_sem=sem.at[0], recv_sem=sem.at[1],
                device_id=peer(k), device_id_type=MESH)
            for k in range(1, count)
        ]

    def finish(src, dst, sem, peer):
        all_of = pltpu.make_async_remote_copy(
            src_ref=src, dst_ref=dst, send_sem=sem.at[0], recv_sem=sem.at[1],
            device_id=peer(1), device_id_type=MESH)
        all_of.wait_send()
        all_of.wait_recv()

    def to_peer(ref):
        return lambda k: ref.at[lax.rem(me_t + k, tm)]

    most, few = pl.ds(0, tm - 1), pl.ds(0, env - 1)
    for c in sends(lambda k: row, rows.at[me_e], esem, env, env_peer):
        c.start()
    for c in sends(to_peer(tx), rx.at[me_t], tsem, tm, tm_peer):
        c.start()
    for c in loads[3:]:
        c.wait()
    turn[...] = jnp.zeros(turn.shape, F32)
    turn[0:DOF, :] = init[0:DOF, :]
    turn[VOFF : VOFF + DOF, :] = init[DOF : 2 * DOF, :]
    turned = turn[...].T
    for p in range(tm):
        own[p] = turned[p * epd : (p + 1) * epd]
    rows[me_e] = row[...]
    rx[me_t] = tx[me_t]

    ratio = float(SUB)
    to_u = TWO_PI / fine_dt
    high_rows = up8(epd)
    lane_of = lax.broadcasted_iota(jnp.int32, (1, LANES), 1)
    wide_lane = lax.broadcasted_iota(jnp.int32, (high_rows, LANES), 1)

    prow[...] = jnp.zeros(prow.shape, F32)
    for i, ref in enumerate((stiff_r, damp_r, gravity_r, cstiff_r, cdamp_r)):
        for pos in range(PER):
            prow[i : i + 1, pos * DOF : (pos + 1) * DOF] = ref[...]
    stiff, damp, gravity, cstiff, cdamp = (prow[i : i + 1, :] for i in range(5))
    for ref in (ybuf, ubuf, ly, lu):
        ref[...] = jnp.zeros(ref.shape, ref.dtype)
    for half in range(2):
        tail = pl.ds(half * LANES + DEPTH, LANES - DEPTH)
        maps_w[:, tail, :] = jnp.zeros((maps.count, LANES - DEPTH, LANES), BF16)
    rank = lax.broadcasted_iota(jnp.int32, (DEPTH, DOF), 0)
    col = lax.broadcasted_iota(jnp.int32, (DEPTH, DOF), 1)
    for n in range(slices):
        span_n = pl.ds(plan.where[n], DOF)
        ly[:, span_n] = jnp.where(rank == col, 1.0, 0.0)
        lu[:, span_n] = jnp.where(rank == col + VOFF, 1.0, 0.0)

    finish(rows.at[few], rows.at[few], esem, env_peer)
    srow[...] = jnp.sum(rows[...], axis=0) * (1.0 / total_env)
    for c in sends(lambda k: srow, sums.at[me_t], ssem, tm, tm_peer):
        c.start()
    sums[me_t] = srow[...]
    finish(tx.at[most], rx.at[most], tsem, tm_peer)

    def by_lane(values, lanes):
        out = values[0]
        for pos in range(1, len(values)):
            out = jnp.where(lanes >= pos * DOF, values[pos], out)
        return out

    def moved_to(value, shift):
        shift = shift % LANES
        return pltpu.roll(value, shift, 1) if shift else value

    pick_row = lax.broadcasted_iota(jnp.int32, (LANES, steps * LANES), 0)
    pick_col = lax.broadcasted_iota(jnp.int32, (LANES, steps * LANES), 1)
    pick = jnp.where(pick_row == SPARE + pick_col // LANES, 1.0, 0.0).astype(BF16)
    flags = dot(jnp.concatenate(
        [rx[t, 0:high_rows, :] for t in range(tm)], axis=0).astype(BF16), pick)
    for g, (base, members) in enumerate(plan.groups):
        span_g = pl.ds(base, LANES)
        for j in range(HS):
            force, hit = [], []
            for pos, n in enumerate(members):
                src, here = divmod(n, local)
                step = here * HS + j
                first, lane = msg.place(step)
                piece = rx[src, first : first + high_rows, :]
                force.append(moved_to(piece, pos * DOF - lane))
                hit.append(flags[src * high_rows : (src + 1) * high_rows,
                                 step * LANES : (step + 1) * LANES])
            touch = by_lane(hit, wide_lane)[0:epd]
            tq[j, :, span_g] = by_lane(force, wide_lane)[0:epd]
            spring[j, :, span_g] = TWO_PI * stiff + touch * (TWO_PI * cstiff)
            fric[j, :, span_g] = to_u * damp + touch * (to_u * cdamp)

    tall_lane = lax.broadcasted_iota(jnp.int32, (VOFF, LANES), 1)
    for g, (base, members) in enumerate(plan.groups):
        wtmp[...] = jnp.zeros(wtmp.shape, F32)
        for pos, n in enumerate(members):
            src, here = divmod(n, local)
            first, lane = msg.place(steps + here)
            piece = moved_to(rx[src, first : first + VOFF, :], pos * DOF - lane)
            inside = (tall_lane >= pos * DOF) & (tall_lane < (pos + 1) * DOF)
            piece = jnp.where(inside, (fine_dt * fine_dt / TWO_PI) * piece, 0.0)
            wtmp[pl.ds(pos * DOF, DOF), :] = piece[0:DOF]
        high, low = split(wtmp[...])
        wgt[g, 0:LANES, :] = high
        wgt[g, LANES:, :] = low

    finish(sums.at[most], sums.at[most], ssem, tm_peer)
    for g, (base, members) in enumerate(plan.groups):
        span_g = pl.ds(base, LANES)
        for j in range(HS):
            means = []
            for n in members:
                src, here = divmod(n, local)
                step = here * HS + j
                means.append(sums[src, step : step + 1, :])
            mean = by_lane(means, lane_of)
            cspring[j, :, span_g] = TWO_PI * (stiff + gravity + mean * cstiff)
            cfric[j, :, span_g] = to_u * (damp + mean * cdamp)

    def once(part, g):
        return dot(jnp.concatenate([part, part], axis=1), wgt[g])

    def product(force, g):
        high, low = split(force)
        top, rest = wgt[g, 0:LANES, :], wgt[g, LANES:, :]
        weight = jnp.concatenate([
            jnp.concatenate([top, rest], axis=1),
            jnp.concatenate([top, jnp.zeros_like(rest)], axis=1)], axis=0)
        both = dot(jnp.concatenate([high, low], axis=1), weight)
        return both[:, :LANES] + both[:, LANES:]

    scale = jnp.where(lane_of < VOFF, TWO_PI, to_u)
    shrink = jnp.where(lane_of < VOFF, 1.0 / TWO_PI, 1.0 / to_u)

    def joined(y, u, depth):
        gap = jnp.zeros((depth, VOFF - DOF), F32)
        return jnp.concatenate(
            [y, gap, u, jnp.zeros((depth, LANES - VOFF - DOF), F32)], axis=1)

    values = {}

    def keep(index, value):
        values[index] = value
        high, low = split(value)
        maps_w[index, 0:DEPTH, :] = high
        maps_w[index, LANES : LANES + DEPTH, :] = low

    def apply(high, low, index):
        weight = maps_w[index, 0:LANES, :]
        return dot(jnp.concatenate([high, low], axis=1),
                   jnp.concatenate([weight, weight], axis=0)) + dot(high, maps_w[index, LANES:, :])

    start = own[me_t] * shrink
    xs[0] = start
    ybuf[:, pl.ds(plan.where[0], DOF)] = start[:, 0:DOF]
    ubuf[:, pl.ds(plan.where[0], DOF)] = start[:, VOFF : VOFF + DOF]
    spans = [pl.ds(base, LANES) for base, members in plan.groups]
    every = range(len(spans))
    y, u = [ly[:, c] for c in spans], [lu[:, c] for c in spans]
    b, a = [ybuf[:, c] for c in spans], [ubuf[:, c] for c in spans]
    for j in range(HS):
        for g in every:
            c = spans[g]
            known = tq[j, :, c] - cspring[j, :, c] * b[g] - cfric[j, :, c] * a[g]
            unit = -cspring[j, :, c] * y[g] - cfric[j, :, c] * u[g]
            gain = ratio * product(jnp.concatenate([unit, known], axis=0), g)
            u[g] = u[g] + gain[0:DEPTH]
            a[g] = a[g] + gain[DEPTH:]
        for g in every:
            b[g] = b[g] + ratio * a[g]
            y[g] = y[g] + ratio * u[g]
    for g in every:
        ly[:, spans[g]], lu[:, spans[g]] = y[g], u[g]
        by[:, spans[g]], bu[:, spans[g]] = b[g], a[g]
    for n in range(slices):
        cut = pl.ds(plan.where[n], DOF)
        keep(n, joined(ly[:, cut], lu[:, cut], DEPTH))

    def sweep(ends, compose=False):
        ends = list(ends)
        half = 1
        while half < slices:
            for first in range(half, slices, 2 * half):
                state = ends[first - 1]
                for n in range(min(first + half, slices) - 1, first - 1, -1):
                    right = maps.index[first, n]
                    target, left = maps.after.get((half, right), (None, None)) if compose else (None, None)
                    if target is None:
                        ends[n] = ends[n] + apply(*split(state), right)
                    else:
                        both = apply(*split(jnp.concatenate([values[left], state], axis=0)), right)
                        keep(target, both[0:DEPTH])
                        ends[n] = ends[n] + both[DEPTH:]
            if compose:
                for target, left, right in maps.stage[half]:
                    if target not in values:
                        keep(target, apply(*split(values[left]), right))
            half *= 2
        return ends

    def packed(yref, uref, n):
        cut = pl.ds(plan.where[n], DOF)
        return joined(yref[:, cut], uref[:, cut], epd)

    ends = sweep([packed(by, bu, n) for n in range(slices)], True)
    for n in range(slices):
        xs[n + 1] = ends[n]

    unroll = SUB - 1 if len(plan.groups) * SUB <= 256 else 1
    grav = gravity

    def iteration(k, active, sliced):
        for n in sliced:
            cut = pl.ds(plan.where[n], DOF)
            ybuf[:, cut] = xs[n, :, 0:DOF]
            ubuf[:, cut] = xs[n, :, VOFF : VOFF + DOF]
        carry = []
        for g in active:
            cut = pl.ds(plan.groups[g][0], LANES)
            y = ybuf[:, cut]
            carry.append((y, ubuf[:, cut], y - jnp.round(y), jnp.zeros_like(y)))
        carry = tuple(carry)

        def horizon(j, carry):
            def substep(flush, counter, carry):
                result = []
                for g, (y, u, t, rest) in zip(active, carry):
                    cut = pl.ds(plan.groups[g][0], LANES)
                    ahead = y + u
                    base = ahead - jnp.round(ahead)
                    s = t * t
                    s2 = s * s
                    weight = grav * t
                    weight2 = weight * s2
                    linear = ((tq[j, :, cut] + rest) - spring[j, :, cut] * y) - fric[j, :, cut] * u
                    force = linear - weight * (SIN[1] * s + SIN[0])
                    force = force - weight2 * (SIN[3] * s + SIN[2])
                    force = force - (weight2 * s2) * (SIN[5] * s + SIN[4])
                    sent = force.astype(BF16)
                    rest = force - sent.astype(F32)
                    push = once(sent, g)
                    if flush:
                        push = push + once(rest.astype(BF16), g)
                        rest = jnp.zeros_like(rest)
                    result.append((ahead + push, u + push, base + push, rest))
                return tuple(result)

            carry = lax.fori_loop(0, SUB - 1, functools.partial(substep, False), carry, unroll=unroll)
            return substep(True, SUB - 1, carry)

        if unroll > 1:
            for j in range(HS):
                carry = horizon(j, carry)
        else:
            carry = lax.fori_loop(0, HS, horizon, carry)
        for g, (y, u, t, rest) in zip(active, carry):
            cut = pl.ds(plan.groups[g][0], LANES)
            ybuf[:, cut] = y
            ubuf[:, cut] = u
        moved = [packed(ybuf, ubuf, n) - xs[n + 1] if n in sliced else None for n in range(slices)]
        if moved[0] is None:
            moved[0] = jnp.zeros((epd, LANES), F32)
        changes = sweep(moved, None)
        for n in range(slices):
            delta[k, n] = changes[n]
            xs[n + 1] = xs[n + 1] + changes[n]

    groups = range(len(plan.groups))
    iteration(0, groups, range(slices))
    live = [n for g in plan.later for n in plan.groups[g][1]]

    @pl.loop(1, ITERS)
    def _(k):
        iteration(k, plan.later, live)

    span = local * epd
    for t in range(tm):
        parts = [xs[t * local + pos + 1] * scale for pos in range(local)]
        turned = jnp.concatenate(parts, axis=0).T
        otx[t, :, 0:span] = turned[0:VOFF]
        otx[t, :, span : 2 * span] = turned[VOFF:DEPTH]
    for c in sends(to_peer(otx), orx.at[me_t], osem, tm, tm_peer):
        c.start()
    worst = jnp.zeros((high_rows, LANES), F32)
    for k in range(ITERS):
        most_moved = jnp.zeros((epd, 1), F32)
        for n in range(slices):
            real = delta[k, n] * scale
            most_moved = jnp.maximum(most_moved, jnp.sum(real * real, axis=1, keepdims=True))
        corr_t[0:epd, :] = jnp.sqrt(most_moved) + jnp.zeros((epd, LANES), F32)
        worst = jnp.where(wide_lane == k, corr_t[...], worst)
    corr_t[...] = worst
    turned = corr_t[...].T
    ctx[...] = jnp.zeros(ctx.shape, F32)
    ctx[:, 0:high_rows] = turned[0:8]
    for c in sends(lambda k: ctx, crx.at[me_t], csem, tm, tm_peer):
        c.start()
    orx[me_t] = otx[me_t]
    crx[me_t] = ctx[...]
    finish(otx.at[most], orx.at[most], osem, tm_peer)
    finish(crx.at[most], crx.at[most], csem, tm_peer)

    across = LANES // epd
    lanes = lax.broadcasted_iota(jnp.int32, (VOFF, LANES), 1)
    for part in range(2):
        for pos in range(local):
            off = part * span + pos * epd
            for tile in range(env_local // LANES):
                acc = None
                for q in range(across):
                    block_in = orx[tile * across + q]
                    shift = (q * epd - off) % LANES
                    moved = pltpu.roll(block_in, shift, 1) if shift else block_in
                    acc = moved if acc is None else jnp.where(lanes >= q * epd, moved, acc)
                cut = pl.ds(tile * LANES, LANES)
                states_out[part * DOF : (part + 1) * DOF, pos, cut] = acc[0:DOF]
    short = lax.broadcasted_iota(jnp.int32, (8, LANES), 1)
    for tile in range(env_local // LANES):
        acc = None
        for q in range(across):
            moved = moved_to(crx[tile * across + q], q * epd)
            acc = moved if acc is None else jnp.where(short >= q * epd, moved, acc)
        corr_out[:, pl.ds(tile * LANES, LANES)] = acc[0:ITERS]


def emit(states, corrections, states_out, corr_out, sem):
    copies = [
        pltpu.make_async_copy(states, states_out, sem.at[0]),
        pltpu.make_async_copy(corrections, corr_out, sem.at[1]),
    ]
    for c in copies:
        c.start()
    for c in copies:
        c.wait()


def body(tm, env, init_state, torque, contact, mass_inverse, stiffness, damping, gravity,
         contact_stiffness, contact_damping):
    local = mass_inverse.shape[0]
    env_local = init_state.shape[1]
    epd = env_local // tm
    steps = local * HS
    slices = local * tm
    plan = Plan(slices)
    maps = Maps(slices).count
    msg = Message(steps, local, epd)
    vmem = pl.BlockSpec(memory_space=pltpu.VMEM)
    dma = pltpu.SemaphoreType.DMA
    prm = [p.reshape(1, DOF) for p in (stiffness, damping, gravity, contact_stiffness, contact_damping)]
    lanes = plan.lanes
    groups = len(plan.groups)
    big = pltpu.VMEM((epd, lanes), F32)
    both = pltpu.VMEM((HS, epd, lanes), F32)
    thin = pltpu.VMEM((HS, 1, lanes), F32)
    row = (up8(steps), LANES)
    states, corrections = pl.pallas_call(
        functools.partial(kernel, tm, env, local, env_local * env),
        out_shape=(
            pltpu.VMEM((2 * DOF, local, env_local), F32),
            pltpu.VMEM((ITERS, env_local), F32),
        ),
        in_specs=[pl.BlockSpec(memory_space=pl.ANY)] * 9,
        out_specs=(vmem, vmem),
        scratch_shapes=[
            pltpu.VMEM((steps, env_local), jnp.int32),
            pltpu.VMEM((DOF, steps, env_local), F32),
            pltpu.VMEM((DOF, local, DOF), F32),
            pltpu.VMEM((2 * DOF, env_local), F32),
        ] + [pltpu.VMEM((1, DOF), F32)] * 5 + [
            pltpu.VMEM((tm, msg.total, LANES), F32), pltpu.VMEM((tm, msg.total, LANES), F32),
            pltpu.VMEM(row, F32), pltpu.VMEM((env,) + row, F32),
            pltpu.VMEM(row, F32), pltpu.VMEM((tm,) + row, F32),
            pltpu.VMEM((tm, VOFF, LANES), F32), pltpu.VMEM((tm, VOFF, LANES), F32),
            pltpu.VMEM((LANES, env_local), F32),
            pltpu.VMEM((max(msg.rows), LANES), F32),
            pltpu.VMEM((tm, epd, LANES), F32),
            both, both, both, pltpu.VMEM((8, LANES), F32), thin, thin,
            pltpu.VMEM((groups, WIDE, LANES), BF16),
            pltpu.VMEM((LANES, LANES), F32),
            big, big, big, big,
            pltpu.VMEM((DEPTH, lanes), F32), pltpu.VMEM((DEPTH, lanes), F32),
            pltpu.VMEM((maps, WIDE, LANES), BF16),
            pltpu.VMEM((slices + 1, epd, LANES), F32),
            dma((2,)), dma((2,)), dma((2,)), dma((2,)), dma((2,)), dma((9,)),
            pltpu.VMEM((ITERS, slices, epd, LANES), F32),
            pltpu.VMEM((up8(epd), LANES), F32),
            pltpu.VMEM((8, LANES), F32), pltpu.VMEM((tm, 8, LANES), F32),
        ],
        compiler_params=pltpu.CompilerParams(collective_id=0, has_side_effects=True),
        name="parareal",
    )(contact, jnp.transpose(torque, (1, 0, 2)),
      jnp.transpose(mass_inverse, (1, 0, 2)), init_state, *prm)
    states, corrections = pl.pallas_call(
        emit,
        out_shape=(
            jax.ShapeDtypeStruct(states.shape, F32),
            jax.ShapeDtypeStruct(corrections.shape, F32),
        ),
        in_specs=[vmem] * 2,
        out_specs=[pl.BlockSpec(memory_space=pl.ANY)] * 2,
        scratch_shapes=[dma((2,))],
        name="emit",
    )(pltpu.with_memory_space_constraint(states, pltpu.VMEM),
      pltpu.with_memory_space_constraint(corrections, pltpu.VMEM))
    return jnp.transpose(states, (1, 0, 2)), corrections


def solution(mesh):
    placed = (
        P(None, "env"),
        P("tm", None, "env"),
        P("tm", "env"),
        P("tm", None, None),
        P(),
        P(),
        P(),
        P(),
        P(),
    )
    return jax.shard_map(
        functools.partial(body, mesh.shape["tm"], mesh.shape["env"]),
        mesh=mesh,
        in_specs=placed,
        out_specs=(P("tm", None, "env"), P(None, "env")),
        check_vma=False,
    )
```

```python
import functools
import math

import jax
import jax.numpy as jnp
from jax import lax
from jax.experimental import pallas as pl
from jax.experimental.pallas import tpu as pltpu
from jax.sharding import PartitionSpec as P

DOF = 35
HS = 2
SUB = 32
ITERS = 3
LANES = 128
WIDE = 256
VOFF = -(-DOF // 8) * 8
DEPTH = 2 * VOFF
PER = LANES // DOF
SPARE = PER * DOF

step_length = 0.05
fine_dt = step_length / SUB
TWO_PI = 2.0 * math.pi
MESH = pl.DeviceIdType.MESH
F32 = jnp.float32
BF16 = jnp.bfloat16

SIN = (
    6.2831825127387075, -41.34139305306742, 81.59546378559027,
    -76.5727543587307, 41.17302274271854, -12.2199194670916,
)


def up8(n):
    return -(-n // 8) * 8


def split(value):
    high = value.astype(BF16)
    return high, (value - high.astype(F32)).astype(BF16)


def dot(left, right):
    return jnp.dot(left, right, preferred_element_type=F32)


class Plan:
    def __init__(self, slices):
        per = PER
        order = list(range(1, slices)) + [0]
        self.groups = []
        self.where = {}
        for first in range(0, slices, per):
            members = order[first : first + per]
            base = LANES * len(self.groups)
            self.groups.append((base, members))
            for pos, n in enumerate(members):
                self.where[n] = base + pos * DOF
        self.lanes = LANES * len(self.groups)
        self.later = [g for g, (base, members) in enumerate(self.groups) if members != [0]]


class Maps:
    def __init__(self, slices):
        self.index = {(n, n): n for n in range(slices)}
        self.stage = {}
        steps = {}

        def need(first, last):
            if (first, last) in steps or first == last:
                return
            half = 1 << ((last - first).bit_length() - 1)
            need(first, first + half - 1)
            need(first + half, last)
            steps[first, last] = (half, (first, first + half - 1), (first + half, last))

        half = 1
        while half < slices:
            self.stage[half] = []
            for first in range(half, slices, 2 * half):
                for n in range(first, min(first + half, slices)):
                    need(first, n)
            half *= 2
        for key in steps:
            self.index[key] = len(self.index)
        for key, (half, left, right) in steps.items():
            self.stage[half].append((self.index[key], self.index[left], self.index[right]))
        self.count = len(self.index)
        self.after = {
            (half, right): (target, left)
            for half, stage in self.stage.items() for target, left, right in stage
        }


class Message:
    def __init__(self, steps, local, epd):
        self.steps, self.local, self.epd = steps, local, epd
        count = steps + local
        self.tiles = -(-count // PER)
        self.rows = []
        self.start = []
        base = 0
        for tile in range(self.tiles):
            pieces = range(tile * PER, min(count, (tile + 1) * PER))
            tall = any(i >= steps for i in pieces)
            rows = max(up8(epd), up8(DOF)) if tall else up8(epd)
            self.start.append(base)
            self.rows.append(rows)
            base += rows
        self.total = base

    def place(self, piece):
        tile, pos = divmod(piece, PER)
        return self.start[tile], pos * DOF


def kernel(
    tm, env, local, total_env,
    contact_h, torque_h, minv_h, init_h, stiff_h, damp_h, gravity_h, cstiff_h, cdamp_h,
    states_out, corr_out,
    contact, torque, minv, init, stiff_r, damp_r, gravity_r, cstiff_r, cdamp_r,
    tx, rx, row, rows, srow, sums, otx, orx, turn, mtile, own,
    tq, spring, fric, prow, cspring, cfric, wgt, wtmp, ybuf, ubuf, by, bu, ly, lu, maps_w, xs,
    tsem, esem, ssem, osem, csem, isem, delta, corr_t, ctx, crx,
):
    slices = local * tm
    steps = local * HS
    env_local = contact.shape[1]
    epd = env_local // tm
    plan = Plan(slices)
    maps = Maps(slices)
    msg = Message(steps, local, epd)
    me_t = lax.axis_index("tm")
    me_e = lax.axis_index("env")
    barrier = pltpu.get_barrier_semaphore()

    def tm_peer(k):
        return {"tm": lax.rem(me_t + k, tm), "env": me_e}

    def env_peer(k):
        return {"tm": me_t, "env": lax.rem(me_e + k, env)}

    for k in range(1, env):
        pl.semaphore_signal(barrier, inc=1, device_id=env_peer(k), device_id_type=MESH)
    for k in range(1, tm):
        pl.semaphore_signal(barrier, inc=1, device_id=tm_peer(k), device_id_type=MESH)

    pairs = (
        (contact_h, contact), (torque_h, torque), (minv_h, minv), (init_h, init),
        (stiff_h, stiff_r), (damp_h, damp_r), (gravity_h, gravity_r),
        (cstiff_h, cstiff_r), (cdamp_h, cdamp_r),
    )
    loads = [pltpu.make_async_copy(a, b, isem.at[i]) for i, (a, b) in enumerate(pairs)]
    for c in loads:
        c.start()
    loads[0].wait()
    hits = contact[...].astype(F32)
    row[...] = jnp.zeros(row.shape, F32)
    row[0:steps, :] = jnp.broadcast_to(jnp.sum(hits, axis=1, keepdims=True), (steps, LANES))
    for c in loads[1:3]:
        c.wait()

    for tile in range(msg.tiles):
        turn[...] = jnp.zeros(turn.shape, F32)
        mtile[...] = jnp.zeros(mtile.shape, F32)
        for pos in range(PER):
            piece = tile * PER + pos
            if piece < steps:
                turn[pos * DOF : (pos + 1) * DOF, :] = torque[:, piece, :]
            elif piece < steps + local:
                mtile[0:DOF, pos * DOF : (pos + 1) * DOF] = minv[:, piece - steps, :]
        if tile == 0:
            turn[SPARE : SPARE + steps, :] = hits
        turned = turn[...].T
        first, count = msg.start[tile], msg.rows[tile]
        tall = count > up8(epd) or any(
            steps <= i < steps + local for i in range(tile * PER, (tile + 1) * PER))
        for p in range(tm):
            chunk = turned[p * epd : (p + 1) * epd]
            if tall:
                tx[p, first : first + count, :] = mtile[0:count, :]
                tx[p, first : first + epd, :] = tx[p, first : first + epd, :] + chunk
            else:
                tx[p, first : first + epd, :] = chunk

    pl.semaphore_wait(barrier, tm + env - 2)

    def sends(src, dst, sem, count, peer):
        return [
            pltpu.make_async_remote_copy(
                src_ref=src(k), dst_ref=dst, send_sem=sem.at[0], recv_sem=sem.at[1],
                device_id=peer(k), device_id_type=MESH)
            for k in range(1, count)
        ]

    def finish(src, dst, sem, peer):
        all_of = pltpu.make_async_remote_copy(
            src_ref=src, dst_ref=dst, send_sem=sem.at[0], recv_sem=sem.at[1],
            device_id=peer(1), device_id_type=MESH)
        all_of.wait_send()
        all_of.wait_recv()

    def to_peer(ref):
        return lambda k: ref.at[lax.rem(me_t + k, tm)]

    most, few = pl.ds(0, tm - 1), pl.ds(0, env - 1)
    for c in sends(lambda k: row, rows.at[me_e], esem, env, env_peer):
        c.start()
    for c in sends(to_peer(tx), rx.at[me_t], tsem, tm, tm_peer):
        c.start()
    for c in loads[3:]:
        c.wait()
    turn[...] = jnp.zeros(turn.shape, F32)
    turn[0:DOF, :] = init[0:DOF, :]
    turn[VOFF : VOFF + DOF, :] = init[DOF : 2 * DOF, :]
    turned = turn[...].T
    for p in range(tm):
        own[p] = turned[p * epd : (p + 1) * epd]
    rows[me_e] = row[...]
    rx[me_t] = tx[me_t]

    ratio = float(SUB)
    to_u = TWO_PI / fine_dt
    high_rows = up8(epd)
    lane_of = lax.broadcasted_iota(jnp.int32, (1, LANES), 1)
    wide_lane = lax.broadcasted_iota(jnp.int32, (high_rows, LANES), 1)

    prow[...] = jnp.zeros(prow.shape, F32)
    for i, ref in enumerate((stiff_r, damp_r, gravity_r, cstiff_r, cdamp_r)):
        for pos in range(PER):
            prow[i : i + 1, pos * DOF : (pos + 1) * DOF] = ref[...]
    stiff, damp, gravity, cstiff, cdamp = (prow[i : i + 1, :] for i in range(5))
    for ref in (ybuf, ubuf, ly, lu):
        ref[...] = jnp.zeros(ref.shape, ref.dtype)
    for half in range(2):
        tail = pl.ds(half * LANES + DEPTH, LANES - DEPTH)
        maps_w[:, tail, :] = jnp.zeros((maps.count, LANES - DEPTH, LANES), BF16)
    rank = lax.broadcasted_iota(jnp.int32, (DEPTH, DOF), 0)
    col = lax.broadcasted_iota(jnp.int32, (DEPTH, DOF), 1)
    for n in range(slices):
        span_n = pl.ds(plan.where[n], DOF)
        ly[:, span_n] = jnp.where(rank == col, 1.0, 0.0)
        lu[:, span_n] = jnp.where(rank == col + VOFF, 1.0, 0.0)

    finish(rows.at[few], rows.at[few], esem, env_peer)
    srow[...] = jnp.sum(rows[...], axis=0) * (1.0 / total_env)
    for c in sends(lambda k: srow, sums.at[me_t], ssem, tm, tm_peer):
        c.start()
    sums[me_t] = srow[...]
    finish(tx.at[most], rx.at[most], tsem, tm_peer)

    def by_lane(values, lanes):
        out = values[0]
        for pos in range(1, len(values)):
            out = jnp.where(lanes >= pos * DOF, values[pos], out)
        return out

    def moved_to(value, shift):
        shift = shift % LANES
        return pltpu.roll(value, shift, 1) if shift else value

    pick_row = lax.broadcasted_iota(jnp.int32, (LANES, steps * LANES), 0)
    pick_col = lax.broadcasted_iota(jnp.int32, (LANES, steps * LANES), 1)
    pick = jnp.where(pick_row == SPARE + pick_col // LANES, 1.0, 0.0).astype(BF16)
    flags = dot(jnp.concatenate(
        [rx[t, 0:high_rows, :] for t in range(tm)], axis=0).astype(BF16), pick)
    for g, (base, members) in enumerate(plan.groups):
        span_g = pl.ds(base, LANES)
        for j in range(HS):
            force, hit = [], []
            for pos, n in enumerate(members):
                src, here = divmod(n, local)
                step = here * HS + j
                first, lane = msg.place(step)
                piece = rx[src, first : first + high_rows, :]
                force.append(moved_to(piece, pos * DOF - lane))
                hit.append(flags[src * high_rows : (src + 1) * high_rows,
                                 step * LANES : (step + 1) * LANES])
            touch = by_lane(hit, wide_lane)[0:epd]
            tq[j, :, span_g] = by_lane(force, wide_lane)[0:epd]
            spring[j, :, span_g] = TWO_PI * stiff + touch * (TWO_PI * cstiff)
            fric[j, :, span_g] = to_u * damp + touch * (to_u * cdamp)

    tall_lane = lax.broadcasted_iota(jnp.int32, (VOFF, LANES), 1)
    for g, (base, members) in enumerate(plan.groups):
        wtmp[...] = jnp.zeros(wtmp.shape, F32)
        for pos, n in enumerate(members):
            src, here = divmod(n, local)
            first, lane = msg.place(steps + here)
            piece = moved_to(rx[src, first : first + VOFF, :], pos * DOF - lane)
            inside = (tall_lane >= pos * DOF) & (tall_lane < (pos + 1) * DOF)
            piece = jnp.where(inside, (fine_dt * fine_dt / TWO_PI) * piece, 0.0)
            wtmp[pl.ds(pos * DOF, DOF), :] = piece[0:DOF]
        high, low = split(wtmp[...])
        wgt[g, 0:LANES, :] = high
        wgt[g, LANES:, :] = low

    finish(sums.at[most], sums.at[most], ssem, tm_peer)
    for g, (base, members) in enumerate(plan.groups):
        span_g = pl.ds(base, LANES)
        for j in range(HS):
            means = []
            for n in members:
                src, here = divmod(n, local)
                step = here * HS + j
                means.append(sums[src, step : step + 1, :])
            mean = by_lane(means, lane_of)
            cspring[j, :, span_g] = TWO_PI * (stiff + gravity + mean * cstiff)
            cfric[j, :, span_g] = to_u * (damp + mean * cdamp)

    def once(part, g):
        return dot(jnp.concatenate([part, part], axis=1), wgt[g])

    def product(force, g):
        high, low = split(force)
        top, rest = wgt[g, 0:LANES, :], wgt[g, LANES:, :]
        weight = jnp.concatenate([
            jnp.concatenate([top, rest], axis=1),
            jnp.concatenate([top, jnp.zeros_like(rest)], axis=1)], axis=0)
        both = dot(jnp.concatenate([high, low], axis=1), weight)
        return both[:, :LANES] + both[:, LANES:]

    scale = jnp.where(lane_of < VOFF, TWO_PI, to_u)
    shrink = jnp.where(lane_of < VOFF, 1.0 / TWO_PI, 1.0 / to_u)

    def joined(y, u, depth):
        gap = jnp.zeros((depth, VOFF - DOF), F32)
        return jnp.concatenate(
            [y, gap, u, jnp.zeros((depth, LANES - VOFF - DOF), F32)], axis=1)

    values = {}

    def keep(index, value):
        values[index] = value
        high, low = split(value)
        maps_w[index, 0:DEPTH, :] = high
        maps_w[index, LANES : LANES + DEPTH, :] = low

    def apply(high, low, index):
        weight = maps_w[index, 0:LANES, :]
        return dot(jnp.concatenate([high, low], axis=1),
                   jnp.concatenate([weight, weight], axis=0)) + dot(high, maps_w[index, LANES:, :])

    start = own[me_t] * shrink
    xs[0] = start
    ybuf[:, pl.ds(plan.where[0], DOF)] = start[:, 0:DOF]
    ubuf[:, pl.ds(plan.where[0], DOF)] = start[:, VOFF : VOFF + DOF]
    spans = [pl.ds(base, LANES) for base, members in plan.groups]
    every = range(len(spans))
    y, u = [ly[:, c] for c in spans], [lu[:, c] for c in spans]
    b, a = [ybuf[:, c] for c in spans], [ubuf[:, c] for c in spans]
    for j in range(HS):
        for g in every:
            c = spans[g]
            known = tq[j, :, c] - cspring[j, :, c] * b[g] - cfric[j, :, c] * a[g]
            unit = -cspring[j, :, c] * y[g] - cfric[j, :, c] * u[g]
            gain = ratio * product(jnp.concatenate([unit, known], axis=0), g)
            u[g] = u[g] + gain[0:DEPTH]
            a[g] = a[g] + gain[DEPTH:]
        for g in every:
            b[g] = b[g] + ratio * a[g]
            y[g] = y[g] + ratio * u[g]
    for g in every:
        ly[:, spans[g]], lu[:, spans[g]] = y[g], u[g]
        by[:, spans[g]], bu[:, spans[g]] = b[g], a[g]
    for n in range(slices):
        cut = pl.ds(plan.where[n], DOF)
        keep(n, joined(ly[:, cut], lu[:, cut], DEPTH))

    def sweep(ends, compose=False):
        ends = list(ends)
        half = 1
        while half < slices:
            for first in range(half, slices, 2 * half):
                state = ends[first - 1]
                if state is None:
                    continue
                for n in range(min(first + half, slices) - 1, first - 1, -1):
                    right = maps.index[first, n]
                    target, left = maps.after.get((half, right), (None, None)) if compose else (None, None)
                    if target is None:
                        ends[n] = ends[n] + apply(*split(state), right)
                    else:
                        both = apply(*split(jnp.concatenate([values[left], state], axis=0)), right)
                        keep(target, both[0:DEPTH])
                        ends[n] = ends[n] + both[DEPTH:]
            if compose:
                for target, left, right in maps.stage[half]:
                    if target not in values:
                        keep(target, apply(*split(values[left]), right))
            half *= 2
        return ends

    def packed(yref, uref, n):
        cut = pl.ds(plan.where[n], DOF)
        return joined(yref[:, cut], uref[:, cut], epd)

    ends = sweep([packed(by, bu, n) for n in range(slices)], True)
    for n in range(slices):
        xs[n + 1] = ends[n]

    unroll = SUB - 1 if len(plan.groups) * SUB <= 256 else 1
    load = [c * gravity for c in SIN]

    def iteration(k, active, sliced):
        for n in sliced:
            cut = pl.ds(plan.where[n], DOF)
            ybuf[:, cut] = xs[n, :, 0:DOF]
            ubuf[:, cut] = xs[n, :, VOFF : VOFF + DOF]
        carry = []
        for g in active:
            cut = pl.ds(plan.groups[g][0], LANES)
            y = ybuf[:, cut]
            carry.append((y, ubuf[:, cut], y - jnp.round(y), jnp.zeros_like(y)))
        carry = tuple(carry)

        def horizon(j, carry):
            def substep(flush, counter, carry):
                result = []
                for g, (y, u, t, rest) in zip(active, carry):
                    cut = pl.ds(plan.groups[g][0], LANES)
                    ahead = y + u
                    base = ahead - jnp.round(ahead)
                    s = t * t
                    s2 = s * s
                    weight2 = t * s2
                    linear = ((tq[j, :, cut] + rest) - spring[j, :, cut] * y) - fric[j, :, cut] * u
                    force = linear - t * (load[1] * s + load[0])
                    force = force - weight2 * (load[3] * s + load[2])
                    force = force - (weight2 * s2) * (load[5] * s + load[4])
                    sent = force.astype(BF16)
                    rest = force - sent.astype(F32)
                    push = once(sent, g)
                    if flush:
                        push = push + once(rest.astype(BF16), g)
                        rest = jnp.zeros_like(rest)
                    result.append((ahead + push, u + push, base + push, rest))
                return tuple(result)

            carry = lax.fori_loop(0, SUB - 1, functools.partial(substep, False), carry, unroll=unroll)
            return substep(not isinstance(j, int) or j == HS - 1, SUB - 1, carry)

        if unroll > 1:
            for j in range(HS):
                carry = horizon(j, carry)
        else:
            carry = lax.fori_loop(0, HS, horizon, carry)
        for g, (y, u, t, rest) in zip(active, carry):
            cut = pl.ds(plan.groups[g][0], LANES)
            ybuf[:, cut] = y
            ubuf[:, cut] = u
        moved = [packed(ybuf, ubuf, n) - xs[n + 1] if n in sliced else None for n in range(slices)]
        changes = sweep(moved)
        for n in range(slices):
            if changes[n] is None:
                delta[k, n] = jnp.zeros((epd, LANES), F32)
                continue
            delta[k, n] = changes[n]
            xs[n + 1] = xs[n + 1] + changes[n]

    groups = range(len(plan.groups))
    iteration(0, groups, range(slices))
    live = [n for g in plan.later for n in plan.groups[g][1]]

    @pl.loop(1, ITERS)
    def _(k):
        iteration(k, plan.later, live)

    span = local * epd
    for t in range(tm):
        parts = [xs[t * local + pos + 1] * scale for pos in range(local)]
        turned = jnp.concatenate(parts, axis=0).T
        otx[t, :, 0:span] = turned[0:VOFF]
        otx[t, :, span : 2 * span] = turned[VOFF:DEPTH]
    for c in sends(to_peer(otx), orx.at[me_t], osem, tm, tm_peer):
        c.start()
    worst = jnp.zeros((high_rows, LANES), F32)
    for k in range(ITERS):
        most_moved = jnp.zeros((epd, 1), F32)
        for n in range(slices):
            real = delta[k, n] * scale
            most_moved = jnp.maximum(most_moved, jnp.sum(real * real, axis=1, keepdims=True))
        corr_t[0:epd, :] = jnp.sqrt(most_moved) + jnp.zeros((epd, LANES), F32)
        worst = jnp.where(wide_lane == k, corr_t[...], worst)
    corr_t[...] = worst
    turned = corr_t[...].T
    ctx[...] = jnp.zeros(ctx.shape, F32)
    ctx[:, 0:high_rows] = turned[0:8]
    for c in sends(lambda k: ctx, crx.at[me_t], csem, tm, tm_peer):
        c.start()
    orx[me_t] = otx[me_t]
    crx[me_t] = ctx[...]
    finish(otx.at[most], orx.at[most], osem, tm_peer)
    finish(crx.at[most], crx.at[most], csem, tm_peer)

    across = LANES // epd
    lanes = lax.broadcasted_iota(jnp.int32, (VOFF, LANES), 1)
    for part in range(2):
        for pos in range(local):
            off = part * span + pos * epd
            for tile in range(env_local // LANES):
                acc = None
                for q in range(across):
                    block_in = orx[tile * across + q]
                    shift = (q * epd - off) % LANES
                    moved = pltpu.roll(block_in, shift, 1) if shift else block_in
                    acc = moved if acc is None else jnp.where(lanes >= q * epd, moved, acc)
                cut = pl.ds(tile * LANES, LANES)
                states_out[part * DOF : (part + 1) * DOF, pos, cut] = acc[0:DOF]
    short = lax.broadcasted_iota(jnp.int32, (8, LANES), 1)
    for tile in range(env_local // LANES):
        acc = None
        for q in range(across):
            moved = moved_to(crx[tile * across + q], q * epd)
            acc = moved if acc is None else jnp.where(short >= q * epd, moved, acc)
        corr_out[:, pl.ds(tile * LANES, LANES)] = acc[0:ITERS]


def emit(states, corrections, states_out, corr_out, sem):
    copies = [
        pltpu.make_async_copy(states, states_out, sem.at[0]),
        pltpu.make_async_copy(corrections, corr_out, sem.at[1]),
    ]
    for c in copies:
        c.start()
    for c in copies:
        c.wait()


def body(tm, env, init_state, torque, contact, mass_inverse, stiffness, damping, gravity,
         contact_stiffness, contact_damping):
    local = mass_inverse.shape[0]
    env_local = init_state.shape[1]
    epd = env_local // tm
    steps = local * HS
    slices = local * tm
    plan = Plan(slices)
    maps = Maps(slices).count
    msg = Message(steps, local, epd)
    vmem = pl.BlockSpec(memory_space=pltpu.VMEM)
    dma = pltpu.SemaphoreType.DMA
    prm = [p.reshape(1, DOF) for p in (stiffness, damping, gravity, contact_stiffness, contact_damping)]
    lanes = plan.lanes
    groups = len(plan.groups)
    big = pltpu.VMEM((epd, lanes), F32)
    both = pltpu.VMEM((HS, epd, lanes), F32)
    thin = pltpu.VMEM((HS, 1, lanes), F32)
    row = (up8(steps), LANES)
    states, corrections = pl.pallas_call(
        functools.partial(kernel, tm, env, local, env_local * env),
        out_shape=(
            pltpu.VMEM((2 * DOF, local, env_local), F32),
            pltpu.VMEM((ITERS, env_local), F32),
        ),
        in_specs=[pl.BlockSpec(memory_space=pl.ANY)] * 9,
        out_specs=(vmem, vmem),
        scratch_shapes=[
            pltpu.VMEM((steps, env_local), jnp.int32),
            pltpu.VMEM((DOF, steps, env_local), F32),
            pltpu.VMEM((DOF, local, DOF), F32),
            pltpu.VMEM((2 * DOF, env_local), F32),
        ] + [pltpu.VMEM((1, DOF), F32)] * 5 + [
            pltpu.VMEM((tm, msg.total, LANES), F32), pltpu.VMEM((tm, msg.total, LANES), F32),
            pltpu.VMEM(row, F32), pltpu.VMEM((env,) + row, F32),
            pltpu.VMEM(row, F32), pltpu.VMEM((tm,) + row, F32),
            pltpu.VMEM((tm, VOFF, LANES), F32), pltpu.VMEM((tm, VOFF, LANES), F32),
            pltpu.VMEM((LANES, env_local), F32),
            pltpu.VMEM((max(msg.rows), LANES), F32),
            pltpu.VMEM((tm, epd, LANES), F32),
            both, both, both, pltpu.VMEM((8, LANES), F32), thin, thin,
            pltpu.VMEM((groups, WIDE, LANES), BF16),
            pltpu.VMEM((LANES, LANES), F32),
            big, big, big, big,
            pltpu.VMEM((DEPTH, lanes), F32), pltpu.VMEM((DEPTH, lanes), F32),
            pltpu.VMEM((maps, WIDE, LANES), BF16),
            pltpu.VMEM((slices + 1, epd, LANES), F32),
            dma((2,)), dma((2,)), dma((2,)), dma((2,)), dma((2,)), dma((9,)),
            pltpu.VMEM((ITERS, slices, epd, LANES), F32),
            pltpu.VMEM((up8(epd), LANES), F32),
            pltpu.VMEM((8, LANES), F32), pltpu.VMEM((tm, 8, LANES), F32),
        ],
        compiler_params=pltpu.CompilerParams(collective_id=0, has_side_effects=True),
        name="parareal",
    )(contact, jnp.transpose(torque, (1, 0, 2)),
      jnp.transpose(mass_inverse, (1, 0, 2)), init_state, *prm)
    states, corrections = pl.pallas_call(
        emit,
        out_shape=(
            jax.ShapeDtypeStruct(states.shape, F32),
            jax.ShapeDtypeStruct(corrections.shape, F32),
        ),
        in_specs=[vmem] * 2,
        out_specs=[pl.BlockSpec(memory_space=pl.ANY)] * 2,
        scratch_shapes=[dma((2,))],
        name="emit",
    )(pltpu.with_memory_space_constraint(states, pltpu.VMEM),
      pltpu.with_memory_space_constraint(corrections, pltpu.VMEM))
    return jnp.transpose(states, (1, 0, 2)), corrections


def solution(mesh):
    placed = (
        P(None, "env"),
        P("tm", None, "env"),
        P("tm", "env"),
        P("tm", None, None),
        P(),
        P(),
        P(),
        P(),
        P(),
    )
    return jax.shard_map(
        functools.partial(body, mesh.shape["tm"], mesh.shape["env"]),
        mesh=mesh,
        in_specs=placed,
        out_specs=(P("tm", None, "env"), P(None, "env")),
        check_vma=False,
    )
```
